256 devices in a mesh: groups: 2 (over y), ctx: 16 (over z), fsdp: 8 (over x, core).
Axes of the slice: x: 4, y: 2, z: 16, core: 2. Of those that a mesh axis runs over, the one named last changes fastest.
The devices are a block of a 4x16x16 slice.
Arguments:
- patches: bfloat16 [16, 4096, 1024], P(('groups', 'fsdp'), 'ctx'), parts along dimension 0, may hold values from -6 to 6
- segment_ids: int32 [16, 4096], P(('groups', 'fsdp'), 'ctx'), parts along dimension 0, may hold values from 0 to 15, never falling along the last dimension, each value on 1 to 3072 neighbouring positions
- patch_rows: int32 [16, 4096], P(('groups', 'fsdp'), 'ctx'), parts along dimension 0, may hold values from 0 to 63
- patch_cols: int32 [16, 4096], P(('groups', 'fsdp'), 'ctx'), parts along dimension 0, may hold values from 0 to 63
- row_table: bfloat16 [64, 1024], replicated, may hold values from -3 to 3
- col_table: bfloat16 [64, 1024], replicated, may hold values from -3 to 3
- norm_gain: float32 [1024], replicated, may hold values from 0.1 to 1.9
- qkv_weight: bfloat16 [1024, 3072], P('fsdp'), may hold values from -5 to 5
- out_weight: bfloat16 [1024, 1024], P(None, 'fsdp'), may hold values from -0.1875 to 0.1875
Outputs:
- encoded: bfloat16 [16, 4096, 1024], P(('groups', 'fsdp'), 'ctx'), parts along dimension 0
The draws below stay inside these ranges and needn't reach their ends.
There are 2 independent parts, one for each index of `groups`. The reference program is written for one: setup_inputs(seed, part) draws one part's arguments, and reference() takes and returns one part's arrays. A program takes and returns all parts, laid end to end along the dimension named above; an argument that names none is the same for every part. Nothing has to cross between parts.
All inputs are finite; a program needn't handle non-finite values.
Results may differ from the reference program's by a relative error of at most 0.0044.
The reference program's roundings to bfloat16 on the way count: a program that leaves them out, or rounds other values in their place, can miss the bound.
Values may be sent and summed in bfloat16 or wider, within the bound.
A program may use at most 64 MiB of HBM per device.

```python
import math
import jax
import jax.numpy as jnp
import numpy as np
from jax import lax

D = 1024
HEADS = 16
GRID = 64
SEGS = 16
LEN = 4096
SEQS = 8
SEG_MOST = 3072


def draw_qkv_weight(key, part):
    base = jnp.clip(jax.random.normal(key, (D, 3 * D), jnp.float32), -2.5, 2.5) * D ** (-0.5)
    return base.astype(jnp.bfloat16)


def touch_ends(entries, key, smallest, top_value):
    longest = entries.shape.index(max(entries.shape))
    spots = []
    for shift in (0, 1):
        where = [jax.random.randint(jax.random.fold_in(key, axis), (), 0, length) for axis, length in enumerate(entries.shape)]
        where[longest] = (where[longest] + shift) % entries.shape[longest]
        spots.append(tuple(where))
    return entries.at[spots[0]].set(smallest).at[spots[1]].set(top_value)


def levels(stream_key, extent, split, low, high):
    def one(dim, blocks):
        draws = jax.random.uniform(jax.random.fold_in(jax.random.fold_in(stream_key, 6), dim), (blocks,), jnp.float32, low / len(split), high / len(split))
        return jnp.repeat(jnp.exp(draws), extent[dim] // blocks).reshape((-1,) + (1,) * (len(extent) - dim - 1))

    level = one(*split[0])
    for cut in split[1:]:
        level = level * one(*cut)
    return level


def profile(amount, total, bound, lean):
    weights = [(1 << 20) // math.isqrt(rank ** lean) + 1 for rank in range(2, amount + 1)]
    spare, given = total - bound - (amount - 1), [1] * (amount - 1)
    while spare > 0:
        candidates = [i for i in range(amount - 1) if given[i] < bound]
        mass, budget = sum([weights[i] for i in candidates]), spare
        for i in candidates:
            addition = min(bound - given[i], max(1, budget * weights[i] // mass), spare)
            given[i] = given[i] + addition
            spare = spare - addition
    return np.array([bound] + given)


def ragged_sizes(own_key, amount, total, most, lean):
    if amount == 2:
        one = jax.random.randint(own_key, (), max(1, total - most), min(most, total - 1) + 1)
        return jnp.stack([one, total - one])
    tallies = jnp.asarray(profile(amount, total, most, lean), jnp.int32)
    pairs = (amount - 1) // 2
    donor, receiver = tallies[1:1 + 2 * pairs:2], tallies[2:2 + 2 * pairs:2]
    slack = jnp.minimum(donor - 1, most - receiver)
    moved = jax.random.randint(jax.random.fold_in(own_key, 1), (pairs,), 0, 1 << 20) % (slack + 1)
    tallies = tallies.at[1:1 + 2 * pairs:2].set(donor - moved).at[2:2 + 2 * pairs:2].set(receiver + moved)
    return tallies[jax.random.permutation(jax.random.fold_in(own_key, 2), amount)]


def bell_draw(rng, shape, width, limit, split=(), held_as=jnp.bfloat16):
    drawn = jax.random.normal(rng, shape, jnp.float32) * width
    if len(split) > 0:
        drawn = levels(rng, shape, split, -0.22, 0.18) * drawn
    return jnp.clip(drawn, min=-limit, max=limit).astype(held_as)


def setup_inputs(seed: int = 0, part: int = 0) -> dict:
    arg_keys = jax.random.split(jax.random.key(seed), 10)
    part_keys = jax.random.split(jax.random.fold_in(arg_keys[9], part), 10)
    return {
        "patches": bell_draw(part_keys[0], (SEQS, LEN, D), 1.0, 6.0, ((0, 8), (1, 16))),
        "segment_ids": jax.vmap(lambda own: jnp.searchsorted(jnp.cumsum(ragged_sizes(own, SEGS, LEN, SEG_MOST, 2)), jnp.arange(LEN), side="right"))(jax.random.split(part_keys[1], SEQS)).reshape((SEQS, LEN)).astype(jnp.int32),
        "patch_rows": touch_ends(jax.random.randint(part_keys[2], (SEQS, LEN), 0, GRID), jax.random.fold_in(part_keys[2], 1), 0, GRID - 1).astype(jnp.int32),
        "patch_cols": touch_ends(jax.random.randint(part_keys[3], (SEQS, LEN), 0, GRID), jax.random.fold_in(part_keys[3], 1), 0, GRID - 1).astype(jnp.int32),
        "row_table": bell_draw(arg_keys[4], (GRID, D), 0.5, 3.0),
        "col_table": bell_draw(arg_keys[5], (GRID, D), 0.5, 3.0),
        "norm_gain": jnp.clip(1.0 + 0.18 * jax.random.normal(arg_keys[6], (D,), jnp.float32), 0.1, 1.9),
        "qkv_weight": draw_qkv_weight(jax.random.fold_in(arg_keys[9], 71), part),
        "out_weight": bell_draw(arg_keys[8], (D, D), D ** -0.5, 0.1875, ((1, 8),)),
    }


floor_score = -1e+30
epsilon = 1e-06

def reference(patches, segment_ids, patch_rows, patch_cols, row_table, col_table, norm_gain, qkv_weight, out_weight):
    model_width = D
    head_count = HEADS
    head_size = model_width // head_count
    score_scale = 1.0 / head_size ** 0.5
    embedded = patches.astype(jnp.float32) + row_table[patch_rows].astype(jnp.float32) + col_table[patch_cols].astype(jnp.float32)
    average = lax.optimization_barrier(jnp.mean(embedded, axis=-1, keepdims=True))
    centered = embedded - average
    variance = lax.optimization_barrier(jnp.mean(centered * centered, axis=-1, keepdims=True))
    normed = (centered * lax.rsqrt(variance + epsilon) * norm_gain).astype(jnp.bfloat16)
    flat_normed = normed.reshape(-1, model_width)
    qkv = jnp.dot(flat_normed, qkv_weight, preferred_element_type=jnp.float32).astype(jnp.bfloat16)
    qkv = qkv.reshape(SEQS, LEN, 3 * model_width)

    def one_sequence(operands):
        packed, labels = operands
        queries = packed[:, :model_width].reshape(LEN, head_count, head_size).transpose(1, 0, 2)
        key_rows = packed[:, model_width:2 * model_width].reshape(LEN, head_count, head_size).transpose(1, 0, 2)
        value_rows = packed[:, 2 * model_width:].reshape(LEN, head_count, head_size).transpose(1, 0, 2)
        same_segment = labels[:, None] == labels[None, :]

        def one_head(head_operands):
            head_q, head_k, head_v = head_operands
            scores = jnp.dot(head_q, head_k.T, preferred_element_type=jnp.float32) * score_scale
            masked = jnp.where(same_segment, scores, floor_score)
            highest = lax.optimization_barrier(jnp.max(masked, axis=-1, keepdims=True))
            raised = jnp.where(same_segment, jnp.exp(masked - highest), 0.0)
            row_sums = lax.optimization_barrier(jnp.sum(raised, axis=-1, keepdims=True))
            mixed = jnp.dot(raised.astype(jnp.bfloat16), head_v, preferred_element_type=jnp.float32) / row_sums
            return mixed.astype(jnp.bfloat16)
        per_head = lax.map(one_head, (queries, key_rows, value_rows))
        return per_head.transpose(1, 0, 2).reshape(LEN, model_width)
    context = lax.map(one_sequence, (qkv, segment_ids))
    attended = jnp.dot(context.reshape(-1, model_width), out_weight, preferred_element_type=jnp.float32)
    encoded = embedded.reshape(-1, model_width) + attended
    return encoded.astype(jnp.bfloat16).reshape(SEQS, LEN, model_width)
```

```python
import functools

import jax
import jax.numpy as jnp
from jax import lax
from jax.experimental import pallas as pl
from jax.experimental.pallas import tpu as pltpu
from jax.sharding import PartitionSpec as P

HEADS = 16
LANES = 128
epsilon = 1e-06
floor_score = -1e30
MESH = pl.DeviceIdType.MESH
F32 = jnp.float32
BF16 = jnp.bfloat16


def flip(value):
    return pltpu.roll(value, LANES // 2, 1)


def far_first(count, step):
    odd = lax.rem(step, 2)
    return count // 2 + (1 - odd) * (step // 2) - odd * ((step + 1) // 2)


def block_kernel(
    ring,
    shards,
    patches,
    labels,
    patch_rows,
    patch_cols,
    row_table,
    col_table,
    gain,
    w_own,
    ow_own,
    out,
    w_all,
    ow_all,
    onehots,
    embedded,
    normed,
    kv_out,
    kv_in,
    q_out,
    q_in,
    c_out,
    c_in,
    labels_in,
    k_aug,
    scores,
    context,
    w_sent,
    w_come,
    ow_sent,
    ow_come,
    kv_sent,
    kv_come,
    q_sent,
    q_come,
    c_sent,
    c_come,
    l_sent,
    l_come,
):
    tokens, width = patches.shape
    half_tokens = tokens // 2
    depth = w_own.shape[0]
    pairs = width // LANES
    chips = shards // 2
    me = lax.axis_index("ctx")
    shard = lax.axis_index("fsdp")
    chip, core = shard // 2, lax.rem(shard, 2)
    own_pair = me // 2
    partner = 2 * chip + 1 - core

    def mate(k, which):
        return 2 * lax.rem(chip + k, chips) + which

    barrier = pltpu.get_barrier_semaphore()
    for k in range(1, chips):
        pl.semaphore_signal(
            barrier, inc=1, device_id={"fsdp": mate(k, core)}, device_id_type=MESH
        )
    pl.semaphore_signal(barrier, inc=1, device_id={"fsdp": partner}, device_id_type=MESH)

    def greet(k, carry):
        pl.semaphore_signal(
            barrier, inc=1, device_id={"ctx": lax.rem(me + k, ring)}, device_id_type=MESH
        )
        return carry

    lax.fori_loop(1, ring, greet, 0)
    pl.semaphore_wait(barrier, ring - 1 + chips)

    lane = lax.broadcasted_iota(jnp.int32, (half_tokens, LANES), 1)
    low = lane < LANES // 2
    lane_full = lax.broadcasted_iota(jnp.int32, (tokens, LANES), 1)
    low_full = lane_full < LANES // 2

    def columns(tile):
        return pl.ds(pl.multiple_of(tile * LANES, LANES), LANES)

    def w_rows(source):
        return pl.ds(pl.multiple_of(source * depth, depth), depth)

    def w_send(tile, target):
        pltpu.make_async_remote_copy(
            src_ref=w_own.at[:, columns(tile)],
            dst_ref=w_all.at[w_rows(shard), columns(tile)],
            send_sem=w_sent.at[tile],
            recv_sem=w_come.at[tile, shard],
            device_id={"fsdp": target},
            device_id_type=MESH,
        ).start()

    def w_wait(tile, source):
        place = w_all.at[w_rows(source), columns(tile)]
        pltpu.make_async_copy(place, place, w_come.at[tile, source]).wait()

    def w_forward(tile, source):
        place = w_all.at[w_rows(source), columns(tile)]
        pltpu.make_async_remote_copy(
            src_ref=place,
            dst_ref=place,
            send_sem=w_sent.at[tile],
            recv_sem=w_come.at[tile, source],
            device_id={"fsdp": partner},
            device_id_type=MESH,
        ).start()

    def pair_of(step):
        return lax.rem(own_pair + far_first(pairs, step), pairs)

    order = [2, 1, 3] if chips == 4 else list(range(1, chips))

    def spread(tiles):
        for k in order:
            for tile in tiles:
                w_send(tile, mate(k, core))
        for tile in tiles:
            w_send(tile, partner)

    def gather(tiles):
        for k in order[1:] + order[:1]:
            for tile in tiles:
                w_wait(tile, mate(k, core))
                w_forward(tile, mate(k, core))
        for tile in tiles:
            w_wait(tile, partner)
        for k in order[1:] + order[:1]:
            for tile in tiles:
                w_wait(tile, mate(k, 1 - core))

    def kv_tiles(step):
        pair = pair_of(step)
        return pairs + pair, 2 * pairs + pair

    def q_tiles(step):
        return (pair_of(step),)

    for step in range(2):
        spread(kv_tiles(step))

    def tell(k, carry):
        target = lax.rem(me + k, ring)
        pltpu.make_async_remote_copy(
            src_ref=labels,
            dst_ref=labels_in.at[me],
            send_sem=l_sent,
            recv_sem=l_come.at[me],
            device_id={"ctx": target},
            device_id_type=MESH,
        ).start()
        return carry

    lax.fori_loop(1, ring, tell, 0)
    labels_in[me] = labels[...]

    levels = lax.broadcasted_iota(jnp.int32, (LANES, tokens), 0)
    grid_size = row_table.shape[0]
    hit = (levels == patch_rows[...]) | (levels == patch_cols[...] + grid_size)
    onehots[...] = jnp.where(hit, 1.0, 0.0).T.astype(BF16)
    table = jnp.concatenate([row_table[...], col_table[...]], axis=0)
    scale = gain[...]
    strip = 64

    def embed(i, carry):
        rows = pl.ds(pl.multiple_of(i * strip, strip), strip)
        value = patches[rows, :].astype(F32) + jnp.dot(
            onehots[rows, :], table, preferred_element_type=F32
        )
        embedded[rows, :] = value
        average = jnp.mean(value, axis=-1, keepdims=True)
        centered = value - average
        variance = jnp.mean(centered * centered, axis=-1, keepdims=True)
        normed[rows, :] = (centered * lax.rsqrt(variance + epsilon) * scale).astype(BF16)
        return carry

    lax.fori_loop(0, tokens // strip, embed, 0)
    w_all[w_rows(shard), :] = w_own[...]

    def project(tile):
        return jnp.dot(normed[...], w_all[:, columns(tile)], preferred_element_type=F32)

    def deliver(outgoing, incoming, sent, come, target):
        @pl.when(target != me)
        def _():
            pltpu.make_async_remote_copy(
                src_ref=outgoing.at[target],
                dst_ref=incoming.at[me],
                send_sem=sent,
                recv_sem=come.at[me],
                device_id={"ctx": target},
                device_id_type=MESH,
            ).start()

        @pl.when(target == me)
        def _():
            incoming[me] = outgoing[target]

    def kv_step(step, carry):
        @pl.when(step < pairs - 2)
        def _():
            spread(kv_tiles(step + 2))

        @pl.when(step >= pairs - 2)
        def _():
            spread(q_tiles(step + 2 - pairs))

        k_tile, v_tile = kv_tiles(step)
        gather((k_tile, v_tile))
        keys = project(k_tile)
        values = project(v_tile)
        first = 2 * pair_of(step)
        kv_out[first] = jnp.where(low_full, keys, flip(values)).astype(BF16)
        kv_out[first + 1] = jnp.where(low_full, flip(keys), values).astype(BF16)
        deliver(kv_out, kv_in, kv_sent, kv_come, first)
        deliver(kv_out, kv_in, kv_sent, kv_come, first + 1)
        return carry

    lax.fori_loop(0, pairs, kv_step, 0)

    def ow_place(source):
        return ow_all.at[:, columns(source)]

    def ow_wait(source):
        pltpu.make_async_copy(ow_place(source), ow_place(source), ow_come.at[source]).wait()

    score_scale = 1.0 / (LANES // 2) ** 0.5

    def q_step(step, carry):
        @pl.when(step < pairs - 2)
        def _():
            spread(q_tiles(step + 2))

        @pl.when(step == pairs - 2)
        def _():
            for k in order + [0]:
                pltpu.make_async_remote_copy(
                    src_ref=ow_own,
                    dst_ref=ow_place(shard),
                    send_sem=ow_sent,
                    recv_sem=ow_come.at[shard],
                    device_id={"fsdp": mate(k, core) if k else partner},
                    device_id_type=MESH,
                ).start()

        (tile,) = q_tiles(step)
        gather((tile,))
        queries = project(tile) * score_scale
        upper, lower = queries[:half_tokens], queries[half_tokens:]
        first = 2 * pair_of(step)
        q_out[first] = jnp.where(low, upper, flip(lower)).astype(BF16)
        q_out[first + 1] = jnp.where(low, flip(upper), lower).astype(BF16)
        deliver(q_out, q_in, q_sent, q_come, first)
        deliver(q_out, q_in, q_sent, q_come, first + 1)
        return carry

    lax.fori_loop(0, pairs, q_step, 0)

    for k in order:
        ow_wait(mate(k, core))
        pltpu.make_async_remote_copy(
            src_ref=ow_place(mate(k, core)),
            dst_ref=ow_place(mate(k, core)),
            send_sem=ow_sent,
            recv_sem=ow_come.at[mate(k, core)],
            device_id={"fsdp": partner},
            device_id_type=MESH,
        ).start()
    ow_all[:, columns(shard)] = ow_own[...]

    label_levels = levels - LANES // 2

    def token_rows(source):
        return pl.ds(pl.multiple_of(source * tokens, tokens), tokens)

    def label_hits(source):
        return jnp.where(label_levels == labels_in[source], 1.0, 0.0).T

    def widen(i, carry):
        source = lax.rem(me + far_first(ring, i), ring)

        @pl.when(source != me)
        def _():
            pltpu.make_async_copy(labels, labels_in.at[source], l_come.at[source]).wait()
            pltpu.make_async_copy(
                kv_out.at[source], kv_in.at[source], kv_come.at[source]
            ).wait()

        other = jnp.where(label_hits(source) > 0.5, 0.0, floor_score).astype(BF16)
        k_aug[token_rows(source), :] = jnp.where(low_full, kv_in[source], other)
        return carry

    lax.fori_loop(0, ring, widen, 0)

    span = 512
    spans = ring * tokens // span
    per_span = span // tokens

    def attend(i, carry):
        offset = jnp.where(i == 0, 0, far_first(ring, i - 1))
        source = lax.rem(me + offset, ring)

        @pl.when(i > 0)
        def _():
            pltpu.make_async_copy(q_out.at[source], q_in.at[source], q_come.at[source]).wait()

        block = q_in[source].astype(F32)
        hits = label_hits(source)
        upper = jnp.where(low, block, hits[:half_tokens])
        lower = jnp.where(low, flip(block), hits[half_tokens:])
        queries = jnp.concatenate([upper, lower], axis=0).astype(BF16)
        highest = jnp.full((tokens, LANES), -jnp.inf, F32)
        for j in range(spans):
            part = lax.dot_general(
                queries,
                k_aug[pl.ds(j * span, span), :],
                (((1,), (1,)), ((), ())),
                preferred_element_type=F32,
            )
            scores[:, pl.ds(j * span, span)] = part
            for t in range(span // LANES):
                highest = jnp.maximum(highest, part[:, t * LANES : (t + 1) * LANES])
        top = jnp.max(highest, axis=-1, keepdims=True)
        sums = jnp.zeros((tokens, LANES), F32)
        mixed = jnp.zeros((tokens, LANES), F32)
        for j in range(spans):
            raised = jnp.exp(scores[:, pl.ds(j * span, span)] - top)
            for t in range(span // LANES):
                sums = sums + raised[:, t * LANES : (t + 1) * LANES]
            values = kv_in[pl.ds(j * per_span, per_span)].reshape(span, LANES)
            mixed = mixed + jnp.dot(raised.astype(BF16), values, preferred_element_type=F32)
        mixed = mixed / jnp.sum(sums, axis=-1, keepdims=True)
        packed = jnp.where(low, flip(mixed[:half_tokens]), mixed[half_tokens:])
        c_out[source] = packed.astype(BF16)
        deliver(c_out, c_in, c_sent, c_come, source)
        return carry

    lax.fori_loop(0, ring, attend, 0)

    ow_wait(partner)
    for k in order:
        ow_wait(mate(k, 1 - core))

    def collect(i, carry):
        source = lax.rem(me + far_first(ring, i), ring)

        @pl.when(source != me)
        def _():
            pltpu.make_async_copy(c_out.at[source], c_in.at[source], c_come.at[source]).wait()

        return carry

    lax.fori_loop(0, ring, collect, 0)
    for pair in range(pairs):
        left = c_in[2 * pair].astype(F32)
        right = c_in[2 * pair + 1].astype(F32)
        place = pl.ds(pair * LANES, LANES)
        context[pl.ds(0, half_tokens), place] = jnp.where(low, left, flip(right)).astype(BF16)
        context[pl.ds(half_tokens, half_tokens), place] = jnp.where(
            low, flip(left), right
        ).astype(BF16)
    wide = 256

    def finish(i, carry):
        place = pl.ds(pl.multiple_of(i * wide, wide), wide)
        attended = jnp.dot(context[...], ow_all[:, place], preferred_element_type=F32)
        out[:, place] = (embedded[:, place] + attended).astype(BF16)
        return carry

    lax.fori_loop(0, width // wide, finish, 0)

    def drain(tile, carry):
        place = w_all.at[pl.ds(0, (2 * chips - 1) * depth), columns(tile)]
        pltpu.make_async_copy(place, place, w_sent.at[tile]).wait()
        return carry

    lax.fori_loop(0, 3 * pairs, drain, 0)
    place = ow_all.at[:, pl.ds(0, (2 * chips - 1) * LANES)]
    pltpu.make_async_copy(place, place, ow_sent).wait()
    for buffer, sent in ((kv_out, kv_sent), (q_out, q_sent), (c_out, c_sent), (labels_in, l_sent)):
        place = buffer.at[pl.ds(0, ring - 1)]
        pltpu.make_async_copy(place, place, sent).wait()


def body(
    ring,
    shards,
    patches,
    segment_ids,
    patch_rows,
    patch_cols,
    row_table,
    col_table,
    norm_gain,
    qkv_weight,
    out_weight,
):
    _, tokens, width = patches.shape
    pairs = width // LANES
    dma = pltpu.SemaphoreType.DMA
    result = pl.pallas_call(
        functools.partial(block_kernel, ring, shards),
        out_shape=jax.ShapeDtypeStruct((tokens, width), BF16),
        in_specs=[pl.BlockSpec(memory_space=pltpu.VMEM)] * 9,
        out_specs=pl.BlockSpec(memory_space=pltpu.VMEM),
        scratch_shapes=[
            pltpu.VMEM((width, 3 * width), BF16),
            pltpu.VMEM((width, width), BF16),
            pltpu.VMEM((tokens, LANES), BF16),
            pltpu.VMEM((tokens, width), F32),
            pltpu.VMEM((tokens, width), BF16),
            pltpu.VMEM((ring, tokens, LANES), BF16),
            pltpu.VMEM((ring, tokens, LANES), BF16),
            pltpu.VMEM((ring, tokens // 2, LANES), BF16),
            pltpu.VMEM((ring, tokens // 2, LANES), BF16),
            pltpu.VMEM((ring, tokens // 2, LANES), BF16),
            pltpu.VMEM((ring, tokens // 2, LANES), BF16),
            pltpu.VMEM((ring, 1, tokens), jnp.int32),
            pltpu.VMEM((ring * tokens, LANES), BF16),
            pltpu.VMEM((tokens, ring * tokens), F32),
            pltpu.VMEM((tokens, width), BF16),
            dma((3 * pairs,)),
            dma((3 * pairs, shards)),
            dma,
            dma((shards,)),
            dma,
            dma((ring,)),
            dma,
            dma((ring,)),
            dma,
            dma((ring,)),
            dma,
            dma((ring,)),
        ],
        compiler_params=pltpu.CompilerParams(
            collective_id=0, has_side_effects=True, vmem_limit_bytes=60 << 20
        ),
        name="encoder_block",
    )(
        patches[0],
        segment_ids,
        patch_rows,
        patch_cols,
        row_table,
        col_table,
        norm_gain[None],
        qkv_weight,
        out_weight,
    )
    return result[None]


def solution(mesh):
    ring, shards = mesh.shape["ctx"], mesh.shape["fsdp"]
    tokens_spec = P(("groups", "fsdp"), "ctx")
    placed = (
        P(("groups", "fsdp"), "ctx", None),
        tokens_spec,
        tokens_spec,
        tokens_spec,
        P(),
        P(),
        P(),
        P("fsdp", None),
        P(None, "fsdp"),
    )
    return jax.shard_map(
        functools.partial(body, ring, shards),
        mesh=mesh,
        in_specs=placed,
        out_specs=P(("groups", "fsdp"), "ctx", None),
        check_vma=False,
    )
```

```python
import functools

import jax
import jax.numpy as jnp
from jax import lax
from jax.experimental import pallas as pl
from jax.experimental.pallas import tpu as pltpu
from jax.sharding import PartitionSpec as P

HEADS = 16
LANES = 128
epsilon = 1e-06
floor_score = -1e30
MESH = pl.DeviceIdType.MESH
F32 = jnp.float32
BF16 = jnp.bfloat16


def flip(value):
    return pltpu.roll(value, LANES // 2, 1)


def far_first(count, step):
    odd = lax.rem(step, 2)
    return count // 2 + (1 - odd) * (step // 2) - odd * ((step + 1) // 2)


def block_kernel(
    ring,
    shards,
    patches,
    labels,
    patch_rows,
    patch_cols,
    row_table,
    col_table,
    gain,
    w_own,
    ow_own,
    out,
    w_all,
    ow_all,
    onehots,
    embedded,
    normed,
    kv_out,
    kv_in,
    q_out,
    q_in,
    c_out,
    c_in,
    labels_in,
    k_aug,
    scores,
    context,
    w_sent,
    w_come,
    ow_sent,
    ow_come,
    kv_sent,
    kv_come,
    q_sent,
    q_come,
    c_sent,
    c_come,
    l_sent,
    l_come,
    below_here,
    here,
):
    tokens, width = patches.shape
    half_tokens = tokens // 2
    depth = w_own.shape[0]
    pairs = width // LANES
    chips = shards // 2
    me = lax.axis_index("ctx")
    shard = lax.axis_index("fsdp")
    chip, core = shard // 2, lax.rem(shard, 2)
    own_pair = me // 2
    partner = 2 * chip + 1 - core

    def mate(k, which):
        return 2 * lax.rem(chip + k, chips) + which

    barrier = pltpu.get_barrier_semaphore()
    has_below, has_above = me > 0, me < ring - 1

    def greet(**where):
        pl.semaphore_signal(barrier, inc=1, device_id=where, device_id_type=MESH)

    for k in range(1, chips):
        greet(fsdp=mate(k, core))
    greet(fsdp=partner)

    @pl.when(has_below)
    def _():
        greet(ctx=me - 1)

    @pl.when(has_above)
    def _():
        greet(ctx=me + 1)

    neighbours = jnp.where(has_below, 1, 0) + jnp.where(has_above, 1, 0)
    pl.semaphore_wait(barrier, chips + neighbours)

    lane = lax.broadcasted_iota(jnp.int32, (half_tokens, LANES), 1)
    low = lane < LANES // 2
    lane_full = lax.broadcasted_iota(jnp.int32, (tokens, LANES), 1)
    low_full = lane_full < LANES // 2

    def columns(tile):
        return pl.ds(pl.multiple_of(tile * LANES, LANES), LANES)

    def w_rows(source):
        return pl.ds(pl.multiple_of(source * depth, depth), depth)

    def w_send(tile, target):
        pltpu.make_async_remote_copy(
            src_ref=w_own.at[:, columns(tile)],
            dst_ref=w_all.at[w_rows(shard), columns(tile)],
            send_sem=w_sent.at[tile],
            recv_sem=w_come.at[tile, shard],
            device_id={"fsdp": target},
            device_id_type=MESH,
        ).start()

    def w_wait(tile, source):
        place = w_all.at[w_rows(source), columns(tile)]
        pltpu.make_async_copy(place, place, w_come.at[tile, source]).wait()

    def w_forward(tile, source):
        place = w_all.at[w_rows(source), columns(tile)]
        pltpu.make_async_remote_copy(
            src_ref=place,
            dst_ref=place,
            send_sem=w_sent.at[tile],
            recv_sem=w_come.at[tile, source],
            device_id={"fsdp": partner},
            device_id_type=MESH,
        ).start()

    def pair_of(step):
        return lax.rem(own_pair + far_first(pairs, step), pairs)

    order = [2, 1, 3] if chips == 4 else list(range(1, chips))

    def spread(tiles):
        for k in order:
            for tile in tiles:
                w_send(tile, mate(k, core))
        for tile in tiles:
            w_send(tile, partner)

    def gather(tiles):
        for k in order[1:] + order[:1]:
            for tile in tiles:
                w_wait(tile, mate(k, core))
                w_forward(tile, mate(k, core))
        for tile in tiles:
            w_wait(tile, partner)
        for k in order[1:] + order[:1]:
            for tile in tiles:
                w_wait(tile, mate(k, 1 - core))

    def rising_pair(step):
        return jnp.where(step < own_pair, own_pair - 1 - step, step)

    def kv_tiles(step):
        pair = rising_pair(step)
        return pairs + pair, 2 * pairs + pair

    def q_tiles(step):
        return (pair_of(step),)

    for step in range(2):
        spread(kv_tiles(step))

    @pl.when(has_below)
    def _():
        pl.semaphore_wait(below_here, 1)

    @pl.when(has_above)
    def _():
        pl.semaphore_signal(below_here, inc=1, device_id={"ctx": me + 1}, device_id_type=MESH)

    def announce(target, carry):
        @pl.when(target < me)
        def _():
            pl.semaphore_signal(
                here.at[me], inc=1, device_id={"ctx": target}, device_id_type=MESH
            )

        return carry

    lax.fori_loop(0, ring, announce, 0)

    def tell_labels(target):
        @pl.when(target > me)
        def _():
            pl.semaphore_wait(here.at[target], 1)

        @pl.when(target != me)
        def _():
            pltpu.make_async_remote_copy(
                src_ref=labels,
                dst_ref=labels_in.at[me],
                send_sem=l_sent,
                recv_sem=l_come.at[me],
                device_id={"ctx": target},
                device_id_type=MESH,
            ).start()

    labels_in[me] = labels[...]

    levels = lax.broadcasted_iota(jnp.int32, (LANES, tokens), 0)
    grid_size = row_table.shape[0]
    hit = (levels == patch_rows[...]) | (levels == patch_cols[...] + grid_size)
    onehots[...] = jnp.where(hit, 1.0, 0.0).T.astype(BF16)
    table = jnp.concatenate([row_table[...], col_table[...]], axis=0)
    scale = gain[...]
    strip = 64

    def embed(i, carry):
        rows = pl.ds(pl.multiple_of(i * strip, strip), strip)
        value = patches[rows, :].astype(F32) + jnp.dot(
            onehots[rows, :], table, preferred_element_type=F32
        )
        embedded[rows, :] = value
        average = jnp.mean(value, axis=-1, keepdims=True)
        centered = value - average
        variance = jnp.mean(centered * centered, axis=-1, keepdims=True)
        normed[rows, :] = (centered * lax.rsqrt(variance + epsilon) * scale).astype(BF16)
        return carry

    lax.fori_loop(0, tokens // strip, embed, 0)
    w_all[w_rows(shard), :] = w_own[...]

    def project(tile):
        return jnp.dot(normed[...], w_all[:, columns(tile)], preferred_element_type=F32)

    def deliver(outgoing, incoming, sent, come, target):
        @pl.when(target != me)
        def _():
            pltpu.make_async_remote_copy(
                src_ref=outgoing.at[target],
                dst_ref=incoming.at[me],
                send_sem=sent,
                recv_sem=come.at[me],
                device_id={"ctx": target},
                device_id_type=MESH,
            ).start()

        @pl.when(target == me)
        def _():
            incoming[me] = outgoing[target]

    def kv_step(step, carry):
        @pl.when(step < pairs - 2)
        def _():
            spread(kv_tiles(step + 2))

        @pl.when(step >= pairs - 2)
        def _():
            spread(q_tiles(step + 2 - pairs))

        k_tile, v_tile = kv_tiles(step)
        gather((k_tile, v_tile))
        keys = project(k_tile)
        values = project(v_tile)
        first = 2 * rising_pair(step)
        kv_out[first] = jnp.where(low_full, keys, flip(values)).astype(BF16)
        kv_out[first + 1] = jnp.where(low_full, flip(keys), values).astype(BF16)
        for target in (first, first + 1):
            tell_labels(target)
            deliver(kv_out, kv_in, kv_sent, kv_come, target)
        return carry

    lax.fori_loop(0, pairs, kv_step, 0)

    def ow_place(source):
        return ow_all.at[:, columns(source)]

    def ow_wait(source):
        pltpu.make_async_copy(ow_place(source), ow_place(source), ow_come.at[source]).wait()

    score_scale = 1.0 / (LANES // 2) ** 0.5

    def q_step(step, carry):
        @pl.when(step < pairs - 2)
        def _():
            spread(q_tiles(step + 2))

        @pl.when(step == pairs - 2)
        def _():
            for k in order + [0]:
                pltpu.make_async_remote_copy(
                    src_ref=ow_own,
                    dst_ref=ow_place(shard),
                    send_sem=ow_sent,
                    recv_sem=ow_come.at[shard],
                    device_id={"fsdp": mate(k, core) if k else partner},
                    device_id_type=MESH,
                ).start()

        (tile,) = q_tiles(step)
        gather((tile,))
        queries = project(tile) * score_scale
        upper, lower = queries[:half_tokens], queries[half_tokens:]
        first = 2 * pair_of(step)
        q_out[first] = jnp.where(low, upper, flip(lower)).astype(BF16)
        q_out[first + 1] = jnp.where(low, flip(upper), lower).astype(BF16)
        deliver(q_out, q_in, q_sent, q_come, first)
        deliver(q_out, q_in, q_sent, q_come, first + 1)
        return carry

    lax.fori_loop(0, pairs, q_step, 0)

    for k in order:
        ow_wait(mate(k, core))
        pltpu.make_async_remote_copy(
            src_ref=ow_place(mate(k, core)),
            dst_ref=ow_place(mate(k, core)),
            send_sem=ow_sent,
            recv_sem=ow_come.at[mate(k, core)],
            device_id={"fsdp": partner},
            device_id_type=MESH,
        ).start()
    ow_all[:, columns(shard)] = ow_own[...]

    label_levels = levels - LANES // 2

    def token_rows(source):
        return pl.ds(pl.multiple_of(source * tokens, tokens), tokens)

    def label_hits(source):
        return jnp.where(label_levels == labels_in[source], 1.0, 0.0).T

    def widen(source, carry):
        @pl.when(source != me)
        def _():
            pltpu.make_async_copy(labels, labels_in.at[source], l_come.at[source]).wait()
            pltpu.make_async_copy(
                kv_out.at[source], kv_in.at[source], kv_come.at[source]
            ).wait()

        other = jnp.where(label_hits(source) > 0.5, 0.0, floor_score).astype(BF16)
        k_aug[token_rows(source), :] = jnp.where(low_full, kv_in[source], other)
        return carry

    lax.fori_loop(0, ring, widen, 0)

    span = 512
    spans = ring * tokens // span
    per_span = span // tokens

    def attend(i, carry):
        source = jnp.where(i == 0, me, jnp.where(i <= me, i - 1, i))

        @pl.when(i > 0)
        def _():
            pltpu.make_async_copy(q_out.at[source], q_in.at[source], q_come.at[source]).wait()

        block = q_in[source].astype(F32)
        hits = label_hits(source)
        upper = jnp.where(low, block, hits[:half_tokens])
        lower = jnp.where(low, flip(block), hits[half_tokens:])
        queries = jnp.concatenate([upper, lower], axis=0).astype(BF16)
        highest = jnp.full((tokens, LANES), -jnp.inf, F32)
        for j in range(spans):
            part = lax.dot_general(
                queries,
                k_aug[pl.ds(j * span, span), :],
                (((1,), (1,)), ((), ())),
                preferred_element_type=F32,
            )
            scores[:, pl.ds(j * span, span)] = part
            for t in range(span // LANES):
                highest = jnp.maximum(highest, part[:, t * LANES : (t + 1) * LANES])
        top = jnp.max(highest, axis=-1, keepdims=True)
        sums = jnp.zeros((tokens, LANES), F32)
        mixed = jnp.zeros((tokens, LANES), F32)
        for j in range(spans):
            raised = jnp.exp(scores[:, pl.ds(j * span, span)] - top)
            for t in range(span // LANES):
                sums = sums + raised[:, t * LANES : (t + 1) * LANES]
            values = kv_in[pl.ds(j * per_span, per_span)].reshape(span, LANES)
            mixed = mixed + jnp.dot(raised.astype(BF16), values, preferred_element_type=F32)
        mixed = mixed / jnp.sum(sums, axis=-1, keepdims=True)
        packed = jnp.where(low, flip(mixed[:half_tokens]), mixed[half_tokens:])
        c_out[source] = packed.astype(BF16)
        deliver(c_out, c_in, c_sent, c_come, source)
        return carry

    lax.fori_loop(0, ring, attend, 0)

    ow_wait(partner)
    for k in order:
        ow_wait(mate(k, 1 - core))

    def collect(i, carry):
        source = lax.rem(me + far_first(ring, i), ring)

        @pl.when(source != me)
        def _():
            pltpu.make_async_copy(c_out.at[source], c_in.at[source], c_come.at[source]).wait()

        return carry

    lax.fori_loop(0, ring, collect, 0)
    for pair in range(pairs):
        left = c_in[2 * pair].astype(F32)
        right = c_in[2 * pair + 1].astype(F32)
        place = pl.ds(pair * LANES, LANES)
        context[pl.ds(0, half_tokens), place] = jnp.where(low, left, flip(right)).astype(BF16)
        context[pl.ds(half_tokens, half_tokens), place] = jnp.where(
            low, flip(left), right
        ).astype(BF16)
    wide = 256

    def finish(i, carry):
        place = pl.ds(pl.multiple_of(i * wide, wide), wide)
        attended = jnp.dot(context[...], ow_all[:, place], preferred_element_type=F32)
        out[:, place] = (embedded[:, place] + attended).astype(BF16)
        return carry

    lax.fori_loop(0, width // wide, finish, 0)

    def drain(tile, carry):
        place = w_all.at[pl.ds(0, (2 * chips - 1) * depth), columns(tile)]
        pltpu.make_async_copy(place, place, w_sent.at[tile]).wait()
        return carry

    lax.fori_loop(0, 3 * pairs, drain, 0)
    place = ow_all.at[:, pl.ds(0, (2 * chips - 1) * LANES)]
    pltpu.make_async_copy(place, place, ow_sent).wait()
    for buffer, sent in ((kv_out, kv_sent), (q_out, q_sent), (c_out, c_sent), (labels_in, l_sent)):
        place = buffer.at[pl.ds(0, ring - 1)]
        pltpu.make_async_copy(place, place, sent).wait()


def body(
    ring,
    shards,
    patches,
    segment_ids,
    patch_rows,
    patch_cols,
    row_table,
    col_table,
    norm_gain,
    qkv_weight,
    out_weight,
):
    _, tokens, width = patches.shape
    pairs = width // LANES
    dma = pltpu.SemaphoreType.DMA
    result = pl.pallas_call(
        functools.partial(block_kernel, ring, shards),
        out_shape=jax.ShapeDtypeStruct((tokens, width), BF16),
        in_specs=[pl.BlockSpec(memory_space=pltpu.VMEM)] * 9,
        out_specs=pl.BlockSpec(memory_space=pltpu.VMEM),
        scratch_shapes=[
            pltpu.VMEM((width, 3 * width), BF16),
            pltpu.VMEM((width, width), BF16),
            pltpu.VMEM((tokens, LANES), BF16),
            pltpu.VMEM((tokens, width), F32),
            pltpu.VMEM((tokens, width), BF16),
            pltpu.VMEM((ring, tokens, LANES), BF16),
            pltpu.VMEM((ring, tokens, LANES), BF16),
            pltpu.VMEM((ring, tokens // 2, LANES), BF16),
            pltpu.VMEM((ring, tokens // 2, LANES), BF16),
            pltpu.VMEM((ring, tokens // 2, LANES), BF16),
            pltpu.VMEM((ring, tokens // 2, LANES), BF16),
            pltpu.VMEM((ring, 1, tokens), jnp.int32),
            pltpu.VMEM((ring * tokens, LANES), BF16),
            pltpu.VMEM((tokens, ring * tokens), F32),
            pltpu.VMEM((tokens, width), BF16),
            dma((3 * pairs,)),
            dma((3 * pairs, shards)),
            dma,
            dma((shards,)),
            dma,
            dma((ring,)),
            dma,
            dma((ring,)),
            dma,
            dma((ring,)),
            dma,
            dma((ring,)),
            pltpu.SemaphoreType.REGULAR,
            pltpu.SemaphoreType.REGULAR((ring,)),
        ],
        compiler_params=pltpu.CompilerParams(
            collective_id=0, has_side_effects=True, vmem_limit_bytes=36 << 20
        ),
        name="encoder_block",
    )(
        patches[0],
        segment_ids,
        patch_rows,
        patch_cols,
        row_table,
        col_table,
        norm_gain[None],
        qkv_weight,
        out_weight,
    )
    return result[None]


def solution(mesh):
    ring, shards = mesh.shape["ctx"], mesh.shape["fsdp"]
    tokens_spec = P(("groups", "fsdp"), "ctx")
    placed = (
        P(("groups", "fsdp"), "ctx", None),
        tokens_spec,
        tokens_spec,
        tokens_spec,
        P(),
        P(),
        P(),
        P("fsdp", None),
        P(None, "fsdp"),
    )
    return jax.shard_map(
        functools.partial(body, ring, shards),
        mesh=mesh,
        in_specs=placed,
        out_specs=P(("groups", "fsdp"), "ctx", None),
        check_vma=False,
    )
```

```python
import functools

import jax
import jax.numpy as jnp
from jax import lax
from jax.experimental import pallas as pl
from jax.experimental.pallas import tpu as pltpu
from jax.sharding import PartitionSpec as P

HEADS = 16
LANES = 128
epsilon = 1e-06
floor_score = -1e30
MESH = pl.DeviceIdType.MESH
F32 = jnp.float32
BF16 = jnp.bfloat16


def flip(value):
    return pltpu.roll(value, LANES // 2, 1)


def far_first(count, step):
    odd = lax.rem(step, 2)
    return count // 2 + (1 - odd) * (step // 2) - odd * ((step + 1) // 2)


def block_kernel(
    ring,
    shards,
    patches_in,
    labels_at,
    rows_at,
    cols_at,
    row_table_in,
    col_table_in,
    gain_in,
    w_in,
    ow_in,
    out,
    patches,
    labels,
    patch_rows,
    patch_cols,
    table,
    gain,
    loaded,
    w_all,
    ow_all,
    onehots,
    embedded,
    normed,
    kv_out,
    kv_in,
    q_out,
    q_in,
    c_out,
    c_in,
    labels_in,
    k_aug,
    scores,
    context,
    w_sent,
    w_come,
    ow_sent,
    ow_come,
    kv_sent,
    kv_come,
    q_sent,
    q_come,
    c_sent,
    c_come,
    l_sent,
    l_come,
    row_here,
    pair_here,
):
    tokens, width = patches.shape
    half_tokens = tokens // 2
    depth = w_in.shape[0]
    pairs = width // LANES
    chips = shards // 2
    me = lax.axis_index("ctx")
    shard = lax.axis_index("fsdp")
    chip, core = shard // 2, lax.rem(shard, 2)
    own_pair = me // 2
    partner = 2 * chip + 1 - core

    def mate(k, which):
        return 2 * lax.rem(chip + k, chips) + which

    def columns(tile):
        return pl.ds(pl.multiple_of(tile * LANES, LANES), LANES)

    def w_rows(source):
        return pl.ds(pl.multiple_of(source * depth, depth), depth)

    def ow_place(source):
        return ow_all.at[:, columns(source)]

    grid_size = row_table_in.shape[0]
    loads = [
        pltpu.make_async_copy(source, target, loaded.at[k])
        for k, (source, target) in enumerate(
            (
                (w_in, w_all.at[w_rows(shard), :]),
                (rows_at, patch_rows),
                (cols_at, patch_cols),
                (row_table_in, table.at[pl.ds(0, grid_size), :]),
                (col_table_in, table.at[pl.ds(grid_size, grid_size), :]),
                (patches_in, patches),
                (gain_in, gain),
                (labels_at, labels),
                (ow_in, ow_place(shard)),
            )
        )
    ]
    for load in loads:
        load.start()

    barrier = pltpu.get_barrier_semaphore()

    def signal(semaphore, **where):
        pl.semaphore_signal(semaphore, inc=1, device_id=where, device_id_type=MESH)

    @pl.when(shard == 0)
    def _():
        pl.semaphore_wait(barrier, shards - 1)
        for other in range(1, shards):
            signal(row_here, fsdp=other)

    @pl.when(shard > 0)
    def _():
        signal(barrier, fsdp=0)
        pl.semaphore_wait(row_here, 1)

    @pl.when(shard > 0)
    def _():
        start = 2 * lax.rem(own_pair + pairs - shard, pairs)
        signal(barrier, ctx=start)
        signal(barrier, ctx=start + 1)

    @pl.when(shard == shards - 1)
    def _():
        signal(barrier, ctx=4 * own_pair + 1 - me)

    def meet(step):
        ahead = far_first(pairs, step)

        @pl.when((shard == ahead) & (shard > 0))
        def _():
            pl.semaphore_wait(barrier, jnp.where(shard == shards - 1, 3, 2))
            for k in range(1, shards):
                signal(pair_here.at[ahead], fsdp=lax.rem(shard + k, shards))

    def met(step):
        ahead = far_first(pairs, step)

        @pl.when((shard != ahead) & (ahead > 0))
        def _():
            pl.semaphore_wait(pair_here.at[ahead], 1)

    lane = lax.broadcasted_iota(jnp.int32, (half_tokens, LANES), 1)
    low = lane < LANES // 2
    lane_full = lax.broadcasted_iota(jnp.int32, (tokens, LANES), 1)
    low_full = lane_full < LANES // 2

    def w_send(tile, target):
        pltpu.make_async_remote_copy(
            src_ref=w_all.at[w_rows(shard), columns(tile)],
            dst_ref=w_all.at[w_rows(shard), columns(tile)],
            send_sem=w_sent.at[tile],
            recv_sem=w_come.at[tile, shard],
            device_id={"fsdp": target},
            device_id_type=MESH,
        ).start()

    def w_wait(tile, source):
        place = w_all.at[w_rows(source), columns(tile)]
        pltpu.make_async_copy(place, place, w_come.at[tile, source]).wait()

    def w_forward(tile, source):
        place = w_all.at[w_rows(source), columns(tile)]
        pltpu.make_async_remote_copy(
            src_ref=place,
            dst_ref=place,
            send_sem=w_sent.at[tile],
            recv_sem=w_come.at[tile, source],
            device_id={"fsdp": partner},
            device_id_type=MESH,
        ).start()

    def pair_of(step):
        return lax.rem(own_pair + far_first(pairs, step), pairs)

    order = [2, 1, 3] if chips == 4 else list(range(1, chips))

    def spread(tiles):
        for k in order:
            for tile in tiles:
                w_send(tile, mate(k, core))
        for tile in tiles:
            w_send(tile, partner)

    def gather(tiles):
        for k in order[1:] + order[:1]:
            for tile in tiles:
                w_wait(tile, mate(k, core))
                w_forward(tile, mate(k, core))
        for tile in tiles:
            w_wait(tile, partner)
        for k in order[1:] + order[:1]:
            for tile in tiles:
                w_wait(tile, mate(k, 1 - core))

    def kv_tiles(step):
        pair = pair_of(step)
        return pairs + pair, 2 * pairs + pair

    def q_tiles(step):
        return (pair_of(step),)

    loads[0].wait()
    for step in range(2):
        spread(kv_tiles(step))

    def tell_labels(target):
        @pl.when(target != me)
        def _():
            pltpu.make_async_remote_copy(
                src_ref=labels,
                dst_ref=labels_in.at[me],
                send_sem=l_sent,
                recv_sem=l_come.at[me],
                device_id={"ctx": target},
                device_id_type=MESH,
            ).start()

    levels = lax.broadcasted_iota(jnp.int32, (LANES, tokens), 0)
    for load in loads[1:]:
        load.wait()
    labels_in[me] = labels[...]
    hit = (levels == patch_rows[...]) | (levels == patch_cols[...] + grid_size)
    onehots[...] = jnp.where(hit, 1.0, 0.0).T.astype(BF16)
    scale = gain[...]
    strip = 64

    def embed(i, carry):
        rows = pl.ds(pl.multiple_of(i * strip, strip), strip)
        value = patches[rows, :].astype(F32) + jnp.dot(
            onehots[rows, :], table[...], preferred_element_type=F32
        )
        embedded[rows, :] = value
        average = jnp.mean(value, axis=-1, keepdims=True)
        centered = value - average
        variance = jnp.mean(centered * centered, axis=-1, keepdims=True)
        normed[rows, :] = (centered * lax.rsqrt(variance + epsilon) * scale).astype(BF16)
        return carry

    lax.fori_loop(0, tokens // strip, embed, 0)

    def project(tile):
        return jnp.dot(normed[...], w_all[:, columns(tile)], preferred_element_type=F32)

    def deliver(outgoing, incoming, sent, come, target):
        @pl.when(target != me)
        def _():
            pltpu.make_async_remote_copy(
                src_ref=outgoing.at[target],
                dst_ref=incoming.at[me],
                send_sem=sent,
                recv_sem=come.at[me],
                device_id={"ctx": target},
                device_id_type=MESH,
            ).start()

        @pl.when(target == me)
        def _():
            incoming[me] = outgoing[target]

    def kv_step(step, carry):
        @pl.when(step < pairs - 2)
        def _():
            spread(kv_tiles(step + 2))

        @pl.when(step >= pairs - 2)
        def _():
            spread(q_tiles(step + 2 - pairs))

        k_tile, v_tile = kv_tiles(step)
        gather((k_tile, v_tile))
        meet(step)
        keys = project(k_tile)
        values = project(v_tile)
        first = 2 * pair_of(step)
        kv_out[first] = jnp.where(low_full, keys, flip(values)).astype(BF16)
        kv_out[first + 1] = jnp.where(low_full, flip(keys), values).astype(BF16)
        met(step)
        for target in (first, first + 1):
            tell_labels(target)
            deliver(kv_out, kv_in, kv_sent, kv_come, target)
        return carry

    lax.fori_loop(0, pairs, kv_step, 0)

    def ow_wait(source):
        pltpu.make_async_copy(ow_place(source), ow_place(source), ow_come.at[source]).wait()

    score_scale = 1.0 / (LANES // 2) ** 0.5

    def q_step(step, carry):
        @pl.when(step < pairs - 2)
        def _():
            spread(q_tiles(step + 2))

        @pl.when(step == pairs - 2)
        def _():
            for k in order + [0]:
                pltpu.make_async_remote_copy(
                    src_ref=ow_place(shard),
                    dst_ref=ow_place(shard),
                    send_sem=ow_sent,
                    recv_sem=ow_come.at[shard],
                    device_id={"fsdp": mate(k, core) if k else partner},
                    device_id_type=MESH,
                ).start()

        (tile,) = q_tiles(step)
        gather((tile,))
        queries = project(tile) * score_scale
        upper, lower = queries[:half_tokens], queries[half_tokens:]
        first = 2 * pair_of(step)
        q_out[first] = jnp.where(low, upper, flip(lower)).astype(BF16)
        q_out[first + 1] = jnp.where(low, flip(upper), lower).astype(BF16)
        deliver(q_out, q_in, q_sent, q_come, first)
        deliver(q_out, q_in, q_sent, q_come, first + 1)
        return carry

    lax.fori_loop(0, pairs, q_step, 0)

    for k in order:
        ow_wait(mate(k, core))
        pltpu.make_async_remote_copy(
            src_ref=ow_place(mate(k, core)),
            dst_ref=ow_place(mate(k, core)),
            send_sem=ow_sent,
            recv_sem=ow_come.at[mate(k, core)],
            device_id={"fsdp": partner},
            device_id_type=MESH,
        ).start()

    label_levels = levels - LANES // 2

    def token_rows(source):
        return pl.ds(pl.multiple_of(source * tokens, tokens), tokens)

    def label_hits(source):
        return jnp.where(label_levels == labels_in[source], 1.0, 0.0).T

    def widen(source, carry):
        @pl.when(source != me)
        def _():
            pltpu.make_async_copy(labels, labels_in.at[source], l_come.at[source]).wait()
            pltpu.make_async_copy(
                kv_out.at[source], kv_in.at[source], kv_come.at[source]
            ).wait()

        other = jnp.where(label_hits(source) > 0.5, 0.0, floor_score).astype(BF16)
        k_aug[token_rows(source), :] = jnp.where(low_full, kv_in[source], other)
        return carry

    lax.fori_loop(0, ring, widen, 0)

    span = 512
    spans = ring * tokens // span
    per_span = span // tokens

    def attend(i, carry):
        offset = jnp.where(i == 0, 0, far_first(ring, i - 1))
        source = lax.rem(me + offset, ring)

        @pl.when(i > 0)
        def _():
            pltpu.make_async_copy(q_out.at[source], q_in.at[source], q_come.at[source]).wait()

        block = q_in[source].astype(F32)
        hits = label_hits(source)
        upper = jnp.where(low, block, hits[:half_tokens])
        lower = jnp.where(low, flip(block), hits[half_tokens:])
        queries = jnp.concatenate([upper, lower], axis=0).astype(BF16)
        highest = jnp.full((tokens, LANES), -jnp.inf, F32)
        for j in range(spans):
            part = lax.dot_general(
                queries,
                k_aug[pl.ds(j * span, span), :],
                (((1,), (1,)), ((), ())),
                preferred_element_type=F32,
            )
            scores[:, pl.ds(j * span, span)] = part
            for t in range(span // LANES):
                highest = jnp.maximum(highest, part[:, t * LANES : (t + 1) * LANES])
        top = jnp.max(highest, axis=-1, keepdims=True)
        sums = jnp.zeros((tokens, LANES), F32)
        mixed = jnp.zeros((tokens, LANES), F32)
        for j in range(spans):
            raised = jnp.exp(scores[:, pl.ds(j * span, span)] - top)
            for t in range(span // LANES):
                sums = sums + raised[:, t * LANES : (t + 1) * LANES]
            values = kv_in[pl.ds(j * per_span, per_span)].reshape(span, LANES)
            mixed = mixed + jnp.dot(raised.astype(BF16), values, preferred_element_type=F32)
        mixed = mixed / jnp.sum(sums, axis=-1, keepdims=True)
        packed = jnp.where(low, flip(mixed[:half_tokens]), mixed[half_tokens:])
        c_out[source] = packed.astype(BF16)
        deliver(c_out, c_in, c_sent, c_come, source)
        return carry

    lax.fori_loop(0, ring, attend, 0)

    ow_wait(partner)
    for k in order:
        ow_wait(mate(k, 1 - core))

    def collect(i, carry):
        source = lax.rem(me + far_first(ring, i), ring)

        @pl.when(source != me)
        def _():
            pltpu.make_async_copy(c_out.at[source], c_in.at[source], c_come.at[source]).wait()

        return carry

    lax.fori_loop(0, ring, collect, 0)
    for pair in range(pairs):
        left = c_in[2 * pair].astype(F32)
        right = c_in[2 * pair + 1].astype(F32)
        place = pl.ds(pair * LANES, LANES)
        context[pl.ds(0, half_tokens), place] = jnp.where(low, left, flip(right)).astype(BF16)
        context[pl.ds(half_tokens, half_tokens), place] = jnp.where(
            low, flip(left), right
        ).astype(BF16)
    wide = 256

    def finish(i, carry):
        place = pl.ds(pl.multiple_of(i * wide, wide), wide)
        attended = jnp.dot(context[...], ow_all[:, place], preferred_element_type=F32)
        out[:, place] = (embedded[:, place] + attended).astype(BF16)
        return carry

    lax.fori_loop(0, width // wide, finish, 0)

    def drain(tile, carry):
        place = w_all.at[pl.ds(0, (2 * chips - 1) * depth), columns(tile)]
        pltpu.make_async_copy(place, place, w_sent.at[tile]).wait()
        return carry

    lax.fori_loop(0, 3 * pairs, drain, 0)
    place = ow_all.at[:, pl.ds(0, (2 * chips - 1) * LANES)]
    pltpu.make_async_copy(place, place, ow_sent).wait()
    for buffer, sent in ((kv_out, kv_sent), (q_out, q_sent), (c_out, c_sent), (labels_in, l_sent)):
        place = buffer.at[pl.ds(0, ring - 1)]
        pltpu.make_async_copy(place, place, sent).wait()


def body(
    ring,
    shards,
    patches,
    segment_ids,
    patch_rows,
    patch_cols,
    row_table,
    col_table,
    norm_gain,
    qkv_weight,
    out_weight,
):
    _, tokens, width = patches.shape
    pairs = width // LANES
    dma = pltpu.SemaphoreType.DMA
    result = pl.pallas_call(
        functools.partial(block_kernel, ring, shards),
        out_shape=jax.ShapeDtypeStruct((tokens, width), BF16),
        in_specs=[pl.BlockSpec(memory_space=pltpu.HBM)] * 9,
        out_specs=pl.BlockSpec(memory_space=pltpu.VMEM),
        scratch_shapes=[
            pltpu.VMEM((tokens, width), BF16),
            pltpu.VMEM((1, tokens), jnp.int32),
            pltpu.VMEM((1, tokens), jnp.int32),
            pltpu.VMEM((1, tokens), jnp.int32),
            pltpu.VMEM((2 * row_table.shape[0], width), BF16),
            pltpu.VMEM((1, width), F32),
            dma((9,)),
            pltpu.VMEM((width, 3 * width), BF16),
            pltpu.VMEM((width, width), BF16),
            pltpu.VMEM((tokens, LANES), BF16),
            pltpu.VMEM((tokens, width), F32),
            pltpu.VMEM((tokens, width), BF16),
            pltpu.VMEM((ring, tokens, LANES), BF16),
            pltpu.VMEM((ring, tokens, LANES), BF16),
            pltpu.VMEM((ring, tokens // 2, LANES), BF16),
            pltpu.VMEM((ring, tokens // 2, LANES), BF16),
            pltpu.VMEM((ring, tokens // 2, LANES), BF16),
            pltpu.VMEM((ring, tokens // 2, LANES), BF16),
            pltpu.VMEM((ring, 1, tokens), jnp.int32),
            pltpu.VMEM((ring * tokens, LANES), BF16),
            pltpu.VMEM((tokens, ring * tokens), F32),
            pltpu.VMEM((tokens, width), BF16),
            dma((3 * pairs,)),
            dma((3 * pairs, shards)),
            dma,
            dma((shards,)),
            dma,
            dma((ring,)),
            dma,
            dma((ring,)),
            dma,
            dma((ring,)),
            dma,
            dma((ring,)),
            pltpu.SemaphoreType.REGULAR,
            pltpu.SemaphoreType.REGULAR((pairs,)),
        ],
        compiler_params=pltpu.CompilerParams(
            collective_id=0, has_side_effects=True, vmem_limit_bytes=60 << 20
        ),
        name="encoder_block",
    )(
        patches[0],
        segment_ids,
        patch_rows,
        patch_cols,
        row_table,
        col_table,
        norm_gain[None],
        qkv_weight,
        out_weight,
    )
    return result[None]


def solution(mesh):
    ring, shards = mesh.shape["ctx"], mesh.shape["fsdp"]
    tokens_spec = P(("groups", "fsdp"), "ctx")
    placed = (
        P(("groups", "fsdp"), "ctx", None),
        tokens_spec,
        tokens_spec,
        tokens_spec,
        P(),
        P(),
        P(),
        P("fsdp", None),
        P(None, "fsdp"),
    )
    return jax.shard_map(
        functools.partial(body, ring, shards),
        mesh=mesh,
        in_specs=placed,
        out_specs=P(("groups", "fsdp"), "ctx", None),
        check_vma=False,
    )
```

```python
import functools

import jax
import jax.numpy as jnp
from jax import lax
from jax.experimental import pallas as pl
from jax.experimental.pallas import tpu as pltpu
from jax.sharding import PartitionSpec as P

HEADS = 16
LANES = 128
epsilon = 1e-06
floor_score = -1e30
MESH = pl.DeviceIdType.MESH
F32 = jnp.float32
BF16 = jnp.bfloat16


def flip(value):
    return pltpu.roll(value, LANES // 2, 1)


def far_first(count, step):
    odd = lax.rem(step, 2)
    return count // 2 + (1 - odd) * (step // 2) - odd * ((step + 1) // 2)


def block_kernel(
    ring,
    shards,
    patches_in,
    labels_at,
    rows_at,
    cols_at,
    row_table_in,
    col_table_in,
    gain_in,
    w_in,
    ow_in,
    out,
    patches,
    labels,
    patch_rows,
    patch_cols,
    table,
    gain,
    loaded,
    w_all,
    ow_all,
    onehots,
    embedded,
    normed,
    kv_out,
    kv_in,
    q_out,
    q_in,
    c_out,
    c_in,
    labels_in,
    k_aug,
    scores,
    context,
    w_sent,
    w_come,
    ow_sent,
    ow_come,
    kv_sent,
    kv_come,
    q_sent,
    q_come,
    c_sent,
    c_come,
    l_sent,
    l_come,
    row_here,
    pair_here,
):
    tokens, width = patches.shape
    half_tokens = tokens // 2
    depth = w_in.shape[0]
    pairs = width // LANES
    chips = shards // 2
    me = lax.axis_index("ctx")
    shard = lax.axis_index("fsdp")
    chip, core = shard // 2, lax.rem(shard, 2)
    own_pair = me // 2
    partner = 2 * chip + 1 - core

    def mate(k, which):
        return 2 * lax.rem(chip + k, chips) + which

    def columns(tile):
        return pl.ds(pl.multiple_of(tile * LANES, LANES), LANES)

    def w_rows(source):
        return pl.ds(pl.multiple_of(source * depth, depth), depth)

    def ow_place(source):
        return ow_all.at[:, columns(source)]

    grid_size = row_table_in.shape[0]
    loads = [
        pltpu.make_async_copy(source, target, loaded.at[k])
        for k, (source, target) in enumerate(
            (
                (w_in, w_all.at[w_rows(shard), :]),
                (rows_at, patch_rows),
                (cols_at, patch_cols),
                (row_table_in, table.at[pl.ds(0, grid_size), :]),
                (col_table_in, table.at[pl.ds(grid_size, grid_size), :]),
                (patches_in, patches),
                (gain_in, gain),
                (labels_at, labels),
                (ow_in, ow_place(shard)),
            )
        )
    ]
    for load in loads:
        load.start()

    barrier = pltpu.get_barrier_semaphore()

    def signal(semaphore, **where):
        pl.semaphore_signal(semaphore, inc=1, device_id=where, device_id_type=MESH)

    @pl.when(shard == 0)
    def _():
        pl.semaphore_wait(barrier, shards - 1)
        for other in range(1, shards):
            signal(row_here, fsdp=other)

    @pl.when(shard > 0)
    def _():
        signal(barrier, fsdp=0)
        pl.semaphore_wait(row_here, 1)

    @pl.when(shard > 0)
    def _():
        start = 2 * lax.rem(own_pair + pairs - shard, pairs)
        signal(barrier, ctx=start)
        signal(barrier, ctx=start + 1)

    @pl.when(shard == shards - 1)
    def _():
        signal(barrier, ctx=4 * own_pair + 1 - me)

    def meet(step):
        ahead = far_first(pairs, step)

        @pl.when((shard == ahead) & (shard > 0))
        def _():
            pl.semaphore_wait(barrier, jnp.where(shard == shards - 1, 3, 2))
            for k in range(1, shards):
                signal(pair_here.at[ahead], fsdp=lax.rem(shard + k, shards))

    def met(step):
        ahead = far_first(pairs, step)

        @pl.when((shard != ahead) & (ahead > 0))
        def _():
            pl.semaphore_wait(pair_here.at[ahead], 1)

    lane = lax.broadcasted_iota(jnp.int32, (half_tokens, LANES), 1)
    low = lane < LANES // 2
    lane_full = lax.broadcasted_iota(jnp.int32, (tokens, LANES), 1)
    low_full = lane_full < LANES // 2

    def w_send(tile, target):
        pltpu.make_async_remote_copy(
            src_ref=w_all.at[w_rows(shard), columns(tile)],
            dst_ref=w_all.at[w_rows(shard), columns(tile)],
            send_sem=w_sent.at[tile],
            recv_sem=w_come.at[tile, shard],
            device_id={"fsdp": target},
            device_id_type=MESH,
        ).start()

    def w_wait(tile, source):
        place = w_all.at[w_rows(source), columns(tile)]
        pltpu.make_async_copy(place, place, w_come.at[tile, source]).wait()

    def w_forward(tile, source):
        place = w_all.at[w_rows(source), columns(tile)]
        pltpu.make_async_remote_copy(
            src_ref=place,
            dst_ref=place,
            send_sem=w_sent.at[tile],
            recv_sem=w_come.at[tile, source],
            device_id={"fsdp": partner},
            device_id_type=MESH,
        ).start()

    def pair_of(step):
        return lax.rem(own_pair + far_first(pairs, step), pairs)

    order = [2, 1, 3] if chips == 4 else list(range(1, chips))

    def spread(tiles):
        for k in order:
            for tile in tiles:
                w_send(tile, mate(k, core))
        for tile in tiles:
            w_send(tile, partner)

    def gather(tiles):
        for k in order[1:] + order[:1]:
            for tile in tiles:
                w_wait(tile, mate(k, core))
                w_forward(tile, mate(k, core))
        for tile in tiles:
            w_wait(tile, partner)
        for k in order[1:] + order[:1]:
            for tile in tiles:
                w_wait(tile, mate(k, 1 - core))

    def kv_tiles(step):
        pair = pair_of(step)
        return pairs + pair, 2 * pairs + pair

    def near_pair(step):
        return pair_of(pairs - 1 - step)

    def q_tiles(step):
        return (near_pair(step),)

    loads[0].wait()
    for step in range(2):
        spread(kv_tiles(step))

    def tell_labels(target):
        @pl.when(target != me)
        def _():
            pltpu.make_async_remote_copy(
                src_ref=labels,
                dst_ref=labels_in.at[me],
                send_sem=l_sent,
                recv_sem=l_come.at[me],
                device_id={"ctx": target},
                device_id_type=MESH,
            ).start()

    levels = lax.broadcasted_iota(jnp.int32, (LANES, tokens), 0)
    for load in loads[1:]:
        load.wait()
    labels_in[me] = labels[...]
    hit = (levels == patch_rows[...]) | (levels == patch_cols[...] + grid_size)
    onehots[...] = jnp.where(hit, 1.0, 0.0).T.astype(BF16)
    scale = gain[...]
    strip = 64

    def embed(i, carry):
        rows = pl.ds(pl.multiple_of(i * strip, strip), strip)
        value = patches[rows, :].astype(F32) + jnp.dot(
            onehots[rows, :], table[...], preferred_element_type=F32
        )
        embedded[rows, :] = value
        average = jnp.mean(value, axis=-1, keepdims=True)
        centered = value - average
        variance = jnp.mean(centered * centered, axis=-1, keepdims=True)
        normed[rows, :] = (centered * lax.rsqrt(variance + epsilon) * scale).astype(BF16)
        return carry

    lax.fori_loop(0, tokens // strip, embed, 0)

    def project(tile):
        return jnp.dot(normed[...], w_all[:, columns(tile)], preferred_element_type=F32)

    def deliver(outgoing, incoming, sent, come, target):
        @pl.when(target != me)
        def _():
            pltpu.make_async_remote_copy(
                src_ref=outgoing.at[target],
                dst_ref=incoming.at[me],
                send_sem=sent,
                recv_sem=come.at[me],
                device_id={"ctx": target},
                device_id_type=MESH,
            ).start()

        @pl.when(target == me)
        def _():
            incoming[me] = outgoing[target]

    def kv_step(step, carry):
        @pl.when(step < pairs - 2)
        def _():
            spread(kv_tiles(step + 2))

        @pl.when(step >= pairs - 2)
        def _():
            spread(q_tiles(step + 2 - pairs))

        k_tile, v_tile = kv_tiles(step)
        gather((k_tile, v_tile))
        meet(step)
        keys = project(k_tile)
        values = project(v_tile)
        first = 2 * pair_of(step)
        kv_out[first] = jnp.where(low_full, keys, flip(values)).astype(BF16)
        kv_out[first + 1] = jnp.where(low_full, flip(keys), values).astype(BF16)
        met(step)
        for target in (first, first + 1):
            tell_labels(target)
            deliver(kv_out, kv_in, kv_sent, kv_come, target)
        return carry

    lax.fori_loop(0, pairs, kv_step, 0)

    def ow_wait(source):
        pltpu.make_async_copy(ow_place(source), ow_place(source), ow_come.at[source]).wait()

    score_scale = 1.0 / (LANES // 2) ** 0.5

    def q_step(step, carry):
        @pl.when(step < pairs - 2)
        def _():
            spread(q_tiles(step + 2))

        @pl.when(step == pairs - 2)
        def _():
            for k in order + [0]:
                pltpu.make_async_remote_copy(
                    src_ref=ow_place(shard),
                    dst_ref=ow_place(shard),
                    send_sem=ow_sent,
                    recv_sem=ow_come.at[shard],
                    device_id={"fsdp": mate(k, core) if k else partner},
                    device_id_type=MESH,
                ).start()

        (tile,) = q_tiles(step)
        gather((tile,))
        queries = project(tile) * score_scale
        upper, lower = queries[:half_tokens], queries[half_tokens:]
        first = 2 * near_pair(step)
        q_out[first] = jnp.where(low, upper, flip(lower)).astype(BF16)
        q_out[first + 1] = jnp.where(low, flip(upper), lower).astype(BF16)
        deliver(q_out, q_in, q_sent, q_come, first)
        deliver(q_out, q_in, q_sent, q_come, first + 1)
        return carry

    lax.fori_loop(0, pairs, q_step, 0)

    def ow_forward():
        for k in order:
            ow_wait(mate(k, core))
            pltpu.make_async_remote_copy(
                src_ref=ow_place(mate(k, core)),
                dst_ref=ow_place(mate(k, core)),
                send_sem=ow_sent,
                recv_sem=ow_come.at[mate(k, core)],
                device_id={"fsdp": partner},
                device_id_type=MESH,
            ).start()

    label_levels = levels - LANES // 2

    def token_rows(source):
        return pl.ds(pl.multiple_of(source * tokens, tokens), tokens)

    def label_hits(source):
        return jnp.where(label_levels == labels_in[source], 1.0, 0.0).T

    def widen(source, carry):
        @pl.when(source != me)
        def _():
            pltpu.make_async_copy(labels, labels_in.at[source], l_come.at[source]).wait()
            pltpu.make_async_copy(
                kv_out.at[source], kv_in.at[source], kv_come.at[source]
            ).wait()

        other = jnp.where(label_hits(source) > 0.5, 0.0, floor_score).astype(BF16)
        k_aug[token_rows(source), :] = jnp.where(low_full, kv_in[source], other)
        return carry

    lax.fori_loop(0, ring, widen, 0)

    everything = ring * tokens

    def attend(i, carry):
        source = lax.rem(me + far_first(ring, ring - 1 - i), ring)

        @pl.when(i == 1)
        def _():
            ow_forward()

        @pl.when(i > 0)
        def _():
            pltpu.make_async_copy(q_out.at[source], q_in.at[source], q_come.at[source]).wait()

        block = q_in[source].astype(F32)
        hits = label_hits(source)
        halves = (
            jnp.where(low, block, hits[:half_tokens]).astype(BF16),
            jnp.where(low, flip(block), hits[half_tokens:]).astype(BF16),
        )

        def score(half):
            part = lax.dot_general(
                halves[half],
                k_aug[...],
                (((1,), (1,)), ((), ())),
                preferred_element_type=F32,
            )
            scores[pl.ds(half * half_tokens, half_tokens), :] = part
            highest = part[:, :LANES]
            for t in range(1, everything // LANES):
                highest = jnp.maximum(highest, part[:, t * LANES : (t + 1) * LANES])
            return jnp.max(highest, axis=-1, keepdims=True)

        def mix(half, top):
            raised = jnp.exp(scores[pl.ds(half * half_tokens, half_tokens), :] - top)
            sums = raised[:, :LANES]
            for t in range(1, everything // LANES):
                sums = sums + raised[:, t * LANES : (t + 1) * LANES]
            mixed = jnp.dot(
                raised.astype(BF16),
                kv_in[...].reshape(everything, LANES),
                preferred_element_type=F32,
            )
            return mixed / jnp.sum(sums, axis=-1, keepdims=True)

        top = score(0)
        next_top = score(1)
        upper = mix(0, top)
        lower = mix(1, next_top)
        c_out[source] = jnp.where(low, flip(upper), lower).astype(BF16)
        deliver(c_out, c_in, c_sent, c_come, source)
        return carry

    lax.fori_loop(0, ring, attend, 0)

    ow_wait(partner)
    for k in order:
        ow_wait(mate(k, 1 - core))

    def collect(i, carry):
        source = lax.rem(me + far_first(ring, i), ring)

        @pl.when(source != me)
        def _():
            pltpu.make_async_copy(c_out.at[source], c_in.at[source], c_come.at[source]).wait()

        return carry

    lax.fori_loop(0, ring, collect, 0)
    for pair in range(pairs):
        left = c_in[2 * pair].astype(F32)
        right = c_in[2 * pair + 1].astype(F32)
        place = pl.ds(pair * LANES, LANES)
        context[pl.ds(0, half_tokens), place] = jnp.where(low, left, flip(right)).astype(BF16)
        context[pl.ds(half_tokens, half_tokens), place] = jnp.where(
            low, flip(left), right
        ).astype(BF16)
    wide = 256

    def finish(i, carry):
        place = pl.ds(pl.multiple_of(i * wide, wide), wide)
        attended = jnp.dot(context[...], ow_all[:, place], preferred_element_type=F32)
        out[:, place] = (embedded[:, place] + attended).astype(BF16)
        return carry

    lax.fori_loop(0, width // wide, finish, 0)

    def drain(tile, carry):
        place = w_all.at[pl.ds(0, (2 * chips - 1) * depth), columns(tile)]
        pltpu.make_async_copy(place, place, w_sent.at[tile]).wait()
        return carry

    lax.fori_loop(0, 3 * pairs, drain, 0)
    place = ow_all.at[:, pl.ds(0, (2 * chips - 1) * LANES)]
    pltpu.make_async_copy(place, place, ow_sent).wait()
    for buffer, sent in ((kv_out, kv_sent), (q_out, q_sent), (c_out, c_sent), (labels_in, l_sent)):
        place = buffer.at[pl.ds(0, ring - 1)]
        pltpu.make_async_copy(place, place, sent).wait()


def body(
    ring,
    shards,
    patches,
    segment_ids,
    patch_rows,
    patch_cols,
    row_table,
    col_table,
    norm_gain,
    qkv_weight,
    out_weight,
):
    _, tokens, width = patches.shape
    pairs = width // LANES
    dma = pltpu.SemaphoreType.DMA
    result = pl.pallas_call(
        functools.partial(block_kernel, ring, shards),
        out_shape=jax.ShapeDtypeStruct((tokens, width), BF16),
        in_specs=[pl.BlockSpec(memory_space=pltpu.HBM)] * 9,
        out_specs=pl.BlockSpec(memory_space=pltpu.VMEM),
        scratch_shapes=[
            pltpu.VMEM((tokens, width), BF16),
            pltpu.VMEM((1, tokens), jnp.int32),
            pltpu.VMEM((1, tokens), jnp.int32),
            pltpu.VMEM((1, tokens), jnp.int32),
            pltpu.VMEM((2 * row_table.shape[0], width), BF16),
            pltpu.VMEM((1, width), F32),
            dma((9,)),
            pltpu.VMEM((width, 3 * width), BF16),
            pltpu.VMEM((width, width), BF16),
            pltpu.VMEM((tokens, LANES), BF16),
            pltpu.VMEM((tokens, width), F32),
            pltpu.VMEM((tokens, width), BF16),
            pltpu.VMEM((ring, tokens, LANES), BF16),
            pltpu.VMEM((ring, tokens, LANES), BF16),
            pltpu.VMEM((ring, tokens // 2, LANES), BF16),
            pltpu.VMEM((ring, tokens // 2, LANES), BF16),
            pltpu.VMEM((ring, tokens // 2, LANES), BF16),
            pltpu.VMEM((ring, tokens // 2, LANES), BF16),
            pltpu.VMEM((ring, 1, tokens), jnp.int32),
            pltpu.VMEM((ring * tokens, LANES), BF16),
            pltpu.VMEM((tokens, ring * tokens), F32),
            pltpu.VMEM((tokens, width), BF16),
            dma((3 * pairs,)),
            dma((3 * pairs, shards)),
            dma,
            dma((shards,)),
            dma,
            dma((ring,)),
            dma,
            dma((ring,)),
            dma,
            dma((ring,)),
            dma,
            dma((ring,)),
            pltpu.SemaphoreType.REGULAR,
            pltpu.SemaphoreType.REGULAR((pairs,)),
        ],
        compiler_params=pltpu.CompilerParams(
            collective_id=0, has_side_effects=True, vmem_limit_bytes=60 << 20
        ),
        name="encoder_block",
    )(
        patches[0],
        segment_ids,
        patch_rows,
        patch_cols,
        row_table,
        col_table,
        norm_gain[None],
        qkv_weight,
        out_weight,
    )
    return result[None]


def solution(mesh):
    ring, shards = mesh.shape["ctx"], mesh.shape["fsdp"]
    tokens_spec = P(("groups", "fsdp"), "ctx")
    placed = (
        P(("groups", "fsdp"), "ctx", None),
        tokens_spec,
        tokens_spec,
        tokens_spec,
        P(),
        P(),
        P(),
        P("fsdp", None),
        P(None, "fsdp"),
    )
    return jax.shard_map(
        functools.partial(body, ring, shards),
        mesh=mesh,
        in_specs=placed,
        out_specs=P(("groups", "fsdp"), "ctx", None),
        check_vma=False,
    )
```

```python
import functools

import jax
import jax.numpy as jnp
from jax import lax
from jax.experimental import pallas as pl
from jax.experimental.pallas import tpu as pltpu
from jax.sharding import PartitionSpec as P

HEADS = 16
LANES = 128
epsilon = 1e-06
floor_score = -1e30
MESH = pl.DeviceIdType.MESH
F32 = jnp.float32
BF16 = jnp.bfloat16


def flip(value):
    return pltpu.roll(value, LANES // 2, 1)


def far_first(count, step):
    odd = lax.rem(step, 2)
    return count // 2 + (1 - odd) * (step // 2) - odd * ((step + 1) // 2)


def block_kernel(
    ring,
    shards,
    patches_in,
    labels_at,
    rows_at,
    cols_at,
    row_table_in,
    col_table_in,
    gain_in,
    w_in,
    ow_in,
    out,
    patches,
    labels,
    patch_rows,
    patch_cols,
    table,
    gain,
    loaded,
    w_all,
    ow_all,
    onehots,
    embedded,
    normed,
    kv_out,
    kv_in,
    q_out,
    q_in,
    c_out,
    c_in,
    labels_in,
    k_aug,
    scores,
    context,
    w_sent,
    mates_come,
    partner_come,
    ow_sent,
    ow_come,
    kv_sent,
    kv_come,
    q_sent,
    q_come,
    c_sent,
    c_come,
    l_sent,
    l_come,
    row_here,
    pair_here,
):
    tokens, width = patches.shape
    half_tokens = tokens // 2
    depth = w_in.shape[0]
    pairs = width // LANES
    chips = shards // 2
    me = lax.axis_index("ctx")
    shard = lax.axis_index("fsdp")
    chip, core = shard // 2, lax.rem(shard, 2)
    own_pair = me // 2
    partner = 2 * chip + 1 - core

    def mate(k, which):
        return 2 * lax.rem(chip + k, chips) + which

    def columns(tile):
        return pl.ds(pl.multiple_of(tile * LANES, LANES), LANES)

    def w_rows(source):
        return pl.ds(pl.multiple_of(source * depth, depth), depth)

    def ow_place(source):
        return ow_all.at[:, columns(source)]

    grid_size = row_table_in.shape[0]
    loads = [
        pltpu.make_async_copy(source, target, loaded.at[k])
        for k, (source, target) in enumerate(
            (
                (w_in, w_all.at[w_rows(shard), :]),
                (rows_at, patch_rows),
                (cols_at, patch_cols),
                (row_table_in, table.at[pl.ds(0, grid_size), :]),
                (col_table_in, table.at[pl.ds(grid_size, grid_size), :]),
                (patches_in, patches),
                (gain_in, gain),
                (labels_at, labels),
                (ow_in, ow_place(shard)),
            )
        )
    ]
    for load in loads:
        load.start()

    barrier = pltpu.get_barrier_semaphore()

    def signal(semaphore, **where):
        pl.semaphore_signal(semaphore, inc=1, device_id=where, device_id_type=MESH)

    @pl.when(shard == 0)
    def _():
        pl.semaphore_wait(barrier, shards - 1)
        for other in range(1, shards):
            signal(row_here, fsdp=other)

    @pl.when(shard > 0)
    def _():
        signal(barrier, fsdp=0)
        pl.semaphore_wait(row_here, 1)

    @pl.when(shard > 0)
    def _():
        start = 2 * lax.rem(own_pair + pairs - shard, pairs)
        signal(barrier, ctx=start)
        signal(barrier, ctx=start + 1)

    @pl.when(shard == shards - 1)
    def _():
        signal(barrier, ctx=4 * own_pair + 1 - me)

    def meet(step):
        ahead = far_first(pairs, step)

        @pl.when((shard == ahead) & (shard > 0))
        def _():
            pl.semaphore_wait(barrier, jnp.where(shard == shards - 1, 3, 2))
            for k in range(1, shards):
                signal(pair_here.at[ahead], fsdp=lax.rem(shard + k, shards))

    def met(step):
        ahead = far_first(pairs, step)

        @pl.when((shard != ahead) & (ahead > 0))
        def _():
            pl.semaphore_wait(pair_here.at[ahead], 1)

    lane = lax.broadcasted_iota(jnp.int32, (half_tokens, LANES), 1)
    low = lane < LANES // 2
    lane_full = lax.broadcasted_iota(jnp.int32, (tokens, LANES), 1)
    low_full = lane_full < LANES // 2

    def pair_of(step):
        return lax.rem(own_pair + far_first(pairs, step), pairs)

    def kv_tiles(step):
        return pairs + pair_of(step), 2 * pairs + pair_of(step)

    def near_then_far(count, near, step):
        return jnp.where(
            step < near, far_first(count, count - 1 - step), far_first(count, step - near)
        )

    def q_pair(step):
        return lax.rem(own_pair + near_then_far(pairs, 3, step), pairs)

    def q_tiles(step):
        return (q_pair(step),)

    order = [2, 1, 3] if chips == 4 else list(range(1, chips))

    def w_copy(source, tile, come, target):
        place = w_all.at[w_rows(source), columns(tile)]
        pltpu.make_async_remote_copy(
            src_ref=place,
            dst_ref=place,
            send_sem=w_sent,
            recv_sem=come,
            device_id={"fsdp": target},
            device_id_type=MESH,
        ).start()

    def spread(number, tiles):
        for k in order:
            for tile in tiles:
                w_copy(shard, tile, mates_come.at[number], mate(k, core))
        for tile in tiles:
            w_copy(shard, tile, partner_come.at[number], partner)

    def w_wait(come, blocks, tiles):
        place = w_all.at[pl.ds(0, blocks * depth), pl.ds(0, len(tiles) * LANES)]
        pltpu.make_async_copy(place, place, come).wait()

    def hand_on(number, tiles):
        w_wait(mates_come.at[number], chips - 1, tiles)
        for k in order:
            for tile in tiles:
                w_copy(mate(k, core), tile, partner_come.at[number], partner)

    def gather(number, tiles):
        w_wait(partner_come.at[number], chips, tiles)

    loads[0].wait()
    for step in range(3):
        spread(step, kv_tiles(step))

    def tell_labels(target):
        @pl.when(target != me)
        def _():
            pltpu.make_async_remote_copy(
                src_ref=labels,
                dst_ref=labels_in.at[me],
                send_sem=l_sent,
                recv_sem=l_come.at[me],
                device_id={"ctx": target},
                device_id_type=MESH,
            ).start()

    levels = lax.broadcasted_iota(jnp.int32, (LANES, tokens), 0)
    for load in loads[1:]:
        load.wait()
    labels_in[me] = labels[...]
    hit = (levels == patch_rows[...]) | (levels == patch_cols[...] + grid_size)
    onehots[...] = jnp.where(hit, 1.0, 0.0).T.astype(BF16)
    scale = gain[...]
    strip = 64

    def embed(i, carry):
        rows = pl.ds(pl.multiple_of(i * strip, strip), strip)
        value = patches[rows, :].astype(F32) + jnp.dot(
            onehots[rows, :], table[...], preferred_element_type=F32
        )
        embedded[rows, :] = value
        average = jnp.mean(value, axis=-1, keepdims=True)
        centered = value - average
        variance = jnp.mean(centered * centered, axis=-1, keepdims=True)
        normed[rows, :] = (centered * lax.rsqrt(variance + epsilon) * scale).astype(BF16)
        return carry

    lax.fori_loop(0, tokens // strip, embed, 0)

    def project(tile):
        return jnp.dot(normed[...], w_all[:, columns(tile)], preferred_element_type=F32)

    def deliver(outgoing, incoming, sent, come, target):
        @pl.when(target != me)
        def _():
            pltpu.make_async_remote_copy(
                src_ref=outgoing.at[target],
                dst_ref=incoming.at[me],
                send_sem=sent,
                recv_sem=come.at[me],
                device_id={"ctx": target},
                device_id_type=MESH,
            ).start()

        @pl.when(target == me)
        def _():
            incoming[me] = outgoing[target]

    hand_on(0, kv_tiles(0))
    meet(0)

    def kv_step(step, carry):
        @pl.when(step < pairs - 3)
        def _():
            spread(step + 3, kv_tiles(step + 3))

        @pl.when(step >= pairs - 3)
        def _():
            spread(step + 3, q_tiles(step + 3 - pairs))

        def next_on():
            @pl.when(step < pairs - 1)
            def _():
                hand_on(step + 1, kv_tiles(step + 1))

            @pl.when(step == pairs - 1)
            def _():
                hand_on(pairs, q_tiles(0))

        k_tile, v_tile = kv_tiles(step)
        gather(step, (k_tile, v_tile))

        @pl.when(step > 0)
        def _():
            next_on()

        keys = project(k_tile)
        values = project(v_tile)
        first = 2 * pair_of(step)
        kv_out[first] = jnp.where(low_full, keys, flip(values)).astype(BF16)
        kv_out[first + 1] = jnp.where(low_full, flip(keys), values).astype(BF16)
        met(step)
        for target in (first, first + 1):
            tell_labels(target)
            deliver(kv_out, kv_in, kv_sent, kv_come, target)

        @pl.when(step == 0)
        def _():
            next_on()

        @pl.when(step < pairs - 1)
        def _():
            meet(step + 1)

        return carry

    lax.fori_loop(0, pairs, kv_step, 0)

    def ow_wait(source):
        pltpu.make_async_copy(ow_place(source), ow_place(source), ow_come.at[source]).wait()

    score_scale = 1.0 / (LANES // 2) ** 0.5

    def q_step(step, carry):
        @pl.when(step < pairs - 3)
        def _():
            spread(pairs + step + 3, q_tiles(step + 3))

        @pl.when(step == pairs - 3)
        def _():
            for k in order + [0]:
                pltpu.make_async_remote_copy(
                    src_ref=ow_place(shard),
                    dst_ref=ow_place(shard),
                    send_sem=ow_sent,
                    recv_sem=ow_come.at[shard],
                    device_id={"fsdp": mate(k, core) if k else partner},
                    device_id_type=MESH,
                ).start()

        (tile,) = q_tiles(step)
        gather(pairs + step, (tile,))

        @pl.when(step < pairs - 1)
        def _():
            hand_on(pairs + step + 1, q_tiles(step + 1))

        queries = project(tile) * score_scale
        upper, lower = queries[:half_tokens], queries[half_tokens:]
        first = 2 * q_pair(step)
        q_out[first] = jnp.where(low, upper, flip(lower)).astype(BF16)
        q_out[first + 1] = jnp.where(low, flip(upper), lower).astype(BF16)
        deliver(q_out, q_in, q_sent, q_come, first)
        deliver(q_out, q_in, q_sent, q_come, first + 1)
        return carry

    lax.fori_loop(0, pairs, q_step, 0)

    def ow_forward():
        for k in order:
            ow_wait(mate(k, core))
            pltpu.make_async_remote_copy(
                src_ref=ow_place(mate(k, core)),
                dst_ref=ow_place(mate(k, core)),
                send_sem=ow_sent,
                recv_sem=ow_come.at[mate(k, core)],
                device_id={"fsdp": partner},
                device_id_type=MESH,
            ).start()

    label_levels = levels - LANES // 2

    def token_rows(source):
        return pl.ds(pl.multiple_of(source * tokens, tokens), tokens)

    def label_hits(source):
        return jnp.where(label_levels == labels_in[source], 1.0, 0.0).T

    def widen(source, carry):
        @pl.when(source != me)
        def _():
            pltpu.make_async_copy(labels, labels_in.at[source], l_come.at[source]).wait()
            pltpu.make_async_copy(
                kv_out.at[source], kv_in.at[source], kv_come.at[source]
            ).wait()

        other = jnp.where(label_hits(source) > 0.5, 0.0, floor_score).astype(BF16)
        k_aug[token_rows(source), :] = jnp.where(low_full, kv_in[source], other)
        return carry

    lax.fori_loop(0, ring, widen, 0)

    everything = ring * tokens

    def attend(i, carry):
        source = lax.rem(me + near_then_far(ring, 5, i), ring)

        @pl.when(i == 1)
        def _():
            ow_forward()

        @pl.when(i > 0)
        def _():
            pltpu.make_async_copy(q_out.at[source], q_in.at[source], q_come.at[source]).wait()

        block = q_in[source].astype(F32)
        hits = label_hits(source)
        halves = (
            jnp.where(low, block, hits[:half_tokens]).astype(BF16),
            jnp.where(low, flip(block), hits[half_tokens:]).astype(BF16),
        )

        def score(half):
            part = lax.dot_general(
                halves[half],
                k_aug[...],
                (((1,), (1,)), ((), ())),
                preferred_element_type=F32,
            )
            scores[pl.ds(half * half_tokens, half_tokens), :] = part
            highest = part[:, :LANES]
            for t in range(1, everything // LANES):
                highest = jnp.maximum(highest, part[:, t * LANES : (t + 1) * LANES])
            return jnp.max(highest, axis=-1, keepdims=True)

        def mix(half, top):
            raised = jnp.exp(scores[pl.ds(half * half_tokens, half_tokens), :] - top)
            sums = raised[:, :LANES]
            for t in range(1, everything // LANES):
                sums = sums + raised[:, t * LANES : (t + 1) * LANES]
            mixed = jnp.dot(
                raised.astype(BF16),
                kv_in[...].reshape(everything, LANES),
                preferred_element_type=F32,
            )
            return mixed / jnp.sum(sums, axis=-1, keepdims=True)

        top = score(0)
        next_top = score(1)
        upper = mix(0, top)
        lower = mix(1, next_top)
        c_out[source] = jnp.where(low, flip(upper), lower).astype(BF16)
        deliver(c_out, c_in, c_sent, c_come, source)
        return carry

    lax.fori_loop(0, ring, attend, 0)

    ow_wait(partner)
    for k in order:
        ow_wait(mate(k, 1 - core))

    def collect(i, carry):
        source = lax.rem(me + far_first(ring, i), ring)

        @pl.when(source != me)
        def _():
            pltpu.make_async_copy(c_out.at[source], c_in.at[source], c_come.at[source]).wait()

        return carry

    lax.fori_loop(0, ring, collect, 0)
    for pair in range(pairs):
        left = c_in[2 * pair].astype(F32)
        right = c_in[2 * pair + 1].astype(F32)
        place = pl.ds(pair * LANES, LANES)
        context[pl.ds(0, half_tokens), place] = jnp.where(low, left, flip(right)).astype(BF16)
        context[pl.ds(half_tokens, half_tokens), place] = jnp.where(
            low, flip(left), right
        ).astype(BF16)
    wide = 256

    def finish(i, carry):
        place = pl.ds(pl.multiple_of(i * wide, wide), wide)
        attended = jnp.dot(context[...], ow_all[:, place], preferred_element_type=F32)
        out[:, place] = (embedded[:, place] + attended).astype(BF16)
        return carry

    lax.fori_loop(0, width // wide, finish, 0)

    place = w_all.at[pl.ds(0, (2 * chips - 1) * depth), :]
    pltpu.make_async_copy(place, place, w_sent).wait()
    place = ow_all.at[:, pl.ds(0, (2 * chips - 1) * LANES)]
    pltpu.make_async_copy(place, place, ow_sent).wait()
    for buffer, sent in ((kv_out, kv_sent), (q_out, q_sent), (c_out, c_sent), (labels_in, l_sent)):
        place = buffer.at[pl.ds(0, ring - 1)]
        pltpu.make_async_copy(place, place, sent).wait()


def body(
    ring,
    shards,
    patches,
    segment_ids,
    patch_rows,
    patch_cols,
    row_table,
    col_table,
    norm_gain,
    qkv_weight,
    out_weight,
):
    _, tokens, width = patches.shape
    pairs = width // LANES
    dma = pltpu.SemaphoreType.DMA
    result = pl.pallas_call(
        functools.partial(block_kernel, ring, shards),
        out_shape=jax.ShapeDtypeStruct((tokens, width), BF16),
        in_specs=[pl.BlockSpec(memory_space=pltpu.HBM)] * 9,
        out_specs=pl.BlockSpec(memory_space=pltpu.VMEM),
        scratch_shapes=[
            pltpu.VMEM((tokens, width), BF16),
            pltpu.VMEM((1, tokens), jnp.int32),
            pltpu.VMEM((1, tokens), jnp.int32),
            pltpu.VMEM((1, tokens), jnp.int32),
            pltpu.VMEM((2 * row_table.shape[0], width), BF16),
            pltpu.VMEM((1, width), F32),
            dma((9,)),
            pltpu.VMEM((width, 3 * width), BF16),
            pltpu.VMEM((width, width), BF16),
            pltpu.VMEM((tokens, LANES), BF16),
            pltpu.VMEM((tokens, width), F32),
            pltpu.VMEM((tokens, width), BF16),
            pltpu.VMEM((ring, tokens, LANES), BF16),
            pltpu.VMEM((ring, tokens, LANES), BF16),
            pltpu.VMEM((ring, tokens // 2, LANES), BF16),
            pltpu.VMEM((ring, tokens // 2, LANES), BF16),
            pltpu.VMEM((ring, tokens // 2, LANES), BF16),
            pltpu.VMEM((ring, tokens // 2, LANES), BF16),
            pltpu.VMEM((ring, 1, tokens), jnp.int32),
            pltpu.VMEM((ring * tokens, LANES), BF16),
            pltpu.VMEM((tokens, ring * tokens), F32),
            pltpu.VMEM((tokens, width), BF16),
            dma,
            dma((2 * pairs,)),
            dma((2 * pairs,)),
            dma,
            dma((shards,)),
            dma,
            dma((ring,)),
            dma,
            dma((ring,)),
            dma,
            dma((ring,)),
            dma,
            dma((ring,)),
            pltpu.SemaphoreType.REGULAR,
            pltpu.SemaphoreType.REGULAR((pairs,)),
        ],
        compiler_params=pltpu.CompilerParams(
            collective_id=0, has_side_effects=True, vmem_limit_bytes=60 << 20
        ),
        name="encoder_block",
    )(
        patches[0],
        segment_ids,
        patch_rows,
        patch_cols,
        row_table,
        col_table,
        norm_gain[None],
        qkv_weight,
        out_weight,
    )
    return result[None]


def solution(mesh):
    ring, shards = mesh.shape["ctx"], mesh.shape["fsdp"]
    tokens_spec = P(("groups", "fsdp"), "ctx")
    placed = (
        P(("groups", "fsdp"), "ctx", None),
        tokens_spec,
        tokens_spec,
        tokens_spec,
        P(),
        P(),
        P(),
        P("fsdp", None),
        P(None, "fsdp"),
    )
    return jax.shard_map(
        functools.partial(body, ring, shards),
        mesh=mesh,
        in_specs=placed,
        out_specs=P(("groups", "fsdp"), "ctx", None),
        check_vma=False,
    )
```

```python
import functools

import jax
import jax.numpy as jnp
from jax import lax
from jax.experimental import pallas as pl
from jax.experimental.pallas import tpu as pltpu
from jax.sharding import PartitionSpec as P

HEADS = 16
LANES = 128
epsilon = 1e-06
floor_score = -1e30
MESH = pl.DeviceIdType.MESH
F32 = jnp.float32
BF16 = jnp.bfloat16


def flip(value):
    return pltpu.roll(value, LANES // 2, 1)


def far_first(count, step):
    odd = lax.rem(step, 2)
    return count // 2 + (1 - odd) * (step // 2) - odd * ((step + 1) // 2)


def block_kernel(
    ring,
    shards,
    patches_in,
    labels_at,
    rows_at,
    cols_at,
    row_table_in,
    col_table_in,
    gain_in,
    w_in,
    ow_in,
    out,
    patches,
    labels,
    patch_rows,
    patch_cols,
    table,
    gain,
    loaded,
    w_all,
    ow_all,
    onehots,
    embedded,
    normed,
    kv_out,
    kv_in,
    q_out,
    q_in,
    c_out,
    c_in,
    labels_in,
    k_aug,
    scores,
    w_sent,
    mates_come,
    partner_come,
    ow_sent,
    ow_come,
    kv_sent,
    kv_come,
    q_sent,
    q_come,
    c_sent,
    c_come,
    l_sent,
    l_come,
    row_here,
    pair_here,
):
    tokens, width = patches.shape
    half_tokens = tokens // 2
    depth = w_in.shape[0]
    pairs = width // LANES
    chips = shards // 2
    me = lax.axis_index("ctx")
    shard = lax.axis_index("fsdp")
    chip, core = shard // 2, lax.rem(shard, 2)
    own_pair = me // 2
    partner = 2 * chip + 1 - core

    def mate(k, which):
        return 2 * lax.rem(chip + k, chips) + which

    def columns(tile):
        return pl.ds(pl.multiple_of(tile * LANES, LANES), LANES)

    def w_rows(source):
        return pl.ds(pl.multiple_of(source * depth, depth), depth)

    def ow_place(source):
        return ow_all.at[:, columns(source)]

    grid_size = row_table_in.shape[0]
    loads = [
        pltpu.make_async_copy(source, target, loaded.at[k])
        for k, (source, target) in enumerate(
            (
                (w_in, w_all.at[w_rows(shard), :]),
                (rows_at, patch_rows),
                (cols_at, patch_cols),
                (row_table_in, table.at[pl.ds(0, grid_size), :]),
                (col_table_in, table.at[pl.ds(grid_size, grid_size), :]),
                (patches_in, patches),
                (gain_in, gain),
                (labels_at, labels),
                (ow_in, ow_place(shard)),
            )
        )
    ]
    for load in loads:
        load.start()

    barrier = pltpu.get_barrier_semaphore()

    def signal(semaphore, **where):
        pl.semaphore_signal(semaphore, inc=1, device_id=where, device_id_type=MESH)

    @pl.when(shard == 0)
    def _():
        pl.semaphore_wait(barrier, shards - 1)
        for other in range(1, shards):
            signal(row_here, fsdp=other)

    @pl.when(shard > 0)
    def _():
        signal(barrier, fsdp=0)
        pl.semaphore_wait(row_here, 1)

    @pl.when(shard > 0)
    def _():
        start = 2 * lax.rem(own_pair + pairs - shard, pairs)
        signal(barrier, ctx=start)
        signal(barrier, ctx=start + 1)

    @pl.when(shard == shards - 1)
    def _():
        signal(barrier, ctx=4 * own_pair + 1 - me)

    def kv_ahead(step):
        return far_first(pairs, jnp.where(step < 2, 1 - step, step))

    def meet(step):
        ahead = kv_ahead(step)

        @pl.when((shard == ahead) & (shard > 0))
        def _():
            pl.semaphore_wait(barrier, jnp.where(shard == shards - 1, 3, 2))
            for k in range(1, shards):
                signal(pair_here.at[ahead], fsdp=lax.rem(shard + k, shards))

    def met(step):
        ahead = kv_ahead(step)

        @pl.when((shard != ahead) & (ahead > 0))
        def _():
            pl.semaphore_wait(pair_here.at[ahead], 1)

    lane = lax.broadcasted_iota(jnp.int32, (half_tokens, LANES), 1)
    low = lane < LANES // 2
    lane_full = lax.broadcasted_iota(jnp.int32, (tokens, LANES), 1)
    low_full = lane_full < LANES // 2

    def pair_of(step):
        return lax.rem(own_pair + kv_ahead(step), pairs)

    def kv_tiles(step):
        return pairs + pair_of(step), 2 * pairs + pair_of(step)

    def near_then_far(count, near, step):
        return jnp.where(
            step < near, far_first(count, count - 1 - step), far_first(count, step - near)
        )

    def q_pair(step):
        return lax.rem(own_pair + near_then_far(pairs, 3, step), pairs)

    def q_tiles(step):
        return (q_pair(step),)

    order = [2, 1, 3] if chips == 4 else list(range(1, chips))

    def w_copy(source, tile, come, target):
        place = w_all.at[w_rows(source), columns(tile)]
        pltpu.make_async_remote_copy(
            src_ref=place,
            dst_ref=place,
            send_sem=w_sent,
            recv_sem=come,
            device_id={"fsdp": target},
            device_id_type=MESH,
        ).start()

    def spread(number, tiles):
        for k in order:
            for tile in tiles:
                w_copy(shard, tile, mates_come.at[number], mate(k, core))
        for tile in tiles:
            w_copy(shard, tile, partner_come.at[number], partner)

    def w_wait(come, blocks, tiles):
        place = w_all.at[pl.ds(0, blocks * depth), pl.ds(0, len(tiles) * LANES)]
        pltpu.make_async_copy(place, place, come).wait()

    def hand_on(number, tiles):
        w_wait(mates_come.at[number], chips - 1, tiles)
        for k in order:
            for tile in tiles:
                w_copy(mate(k, core), tile, partner_come.at[number], partner)

    def gather(number, tiles):
        w_wait(partner_come.at[number], chips, tiles)

    loads[0].wait()
    for step in range(3):
        spread(step, kv_tiles(step))

    def tell_labels(target):
        @pl.when(target != me)
        def _():
            pltpu.make_async_remote_copy(
                src_ref=labels,
                dst_ref=labels_in.at[me],
                send_sem=l_sent,
                recv_sem=l_come.at[me],
                device_id={"ctx": target},
                device_id_type=MESH,
            ).start()

    levels = lax.broadcasted_iota(jnp.int32, (LANES, tokens), 0)
    for load in loads[1:]:
        load.wait()
    labels_in[me] = labels[...]
    hit = (levels == patch_rows[...]) | (levels == patch_cols[...] + grid_size)
    onehots[...] = jnp.where(hit, 1.0, 0.0).T.astype(BF16)
    scale = gain[...]
    strip = 64

    def embed(i, carry):
        rows = pl.ds(pl.multiple_of(i * strip, strip), strip)
        value = patches[rows, :].astype(F32) + jnp.dot(
            onehots[rows, :], table[...], preferred_element_type=F32
        )
        embedded[rows, :] = value
        average = jnp.mean(value, axis=-1, keepdims=True)
        centered = value - average
        variance = jnp.mean(centered * centered, axis=-1, keepdims=True)
        normed[rows, :] = (centered * lax.rsqrt(variance + epsilon) * scale).astype(BF16)
        return carry

    lax.fori_loop(0, tokens // strip, embed, 0)

    def project(tile):
        return jnp.dot(normed[...], w_all[:, columns(tile)], preferred_element_type=F32)

    def deliver(outgoing, incoming, sent, come, target):
        @pl.when(target != me)
        def _():
            pltpu.make_async_remote_copy(
                src_ref=outgoing.at[target],
                dst_ref=incoming.at[me],
                send_sem=sent,
                recv_sem=come.at[me],
                device_id={"ctx": target},
                device_id_type=MESH,
            ).start()

        @pl.when(target == me)
        def _():
            incoming[me] = outgoing[target]

    hand_on(0, kv_tiles(0))
    meet(0)

    def kv_step(step, carry):
        @pl.when(step < pairs - 3)
        def _():
            spread(step + 3, kv_tiles(step + 3))

        @pl.when(step >= pairs - 3)
        def _():
            spread(step + 3, q_tiles(step + 3 - pairs))

        def next_on():
            @pl.when(step < pairs - 1)
            def _():
                hand_on(step + 1, kv_tiles(step + 1))

            @pl.when(step == pairs - 1)
            def _():
                hand_on(pairs, q_tiles(0))

        k_tile, v_tile = kv_tiles(step)
        gather(step, (k_tile, v_tile))

        @pl.when(step > 0)
        def _():
            next_on()

        keys = project(k_tile)
        values = project(v_tile)
        first = 2 * pair_of(step)
        kv_out[first] = jnp.where(low_full, keys, flip(values)).astype(BF16)
        kv_out[first + 1] = jnp.where(low_full, flip(keys), values).astype(BF16)
        met(step)
        for target in (first, first + 1):
            tell_labels(target)
            deliver(kv_out, kv_in, kv_sent, kv_come, target)

        @pl.when(step == 0)
        def _():
            next_on()

        @pl.when(step < pairs - 1)
        def _():
            meet(step + 1)

        return carry

    lax.fori_loop(0, pairs, kv_step, 0)

    def ow_wait(source):
        pltpu.make_async_copy(ow_place(source), ow_place(source), ow_come.at[source]).wait()

    score_scale = 1.0 / (LANES // 2) ** 0.5

    def q_step(step, carry):
        @pl.when(step < pairs - 3)
        def _():
            spread(pairs + step + 3, q_tiles(step + 3))

        @pl.when(step == pairs - 3)
        def _():
            for k in order + [0]:
                pltpu.make_async_remote_copy(
                    src_ref=ow_place(shard),
                    dst_ref=ow_place(shard),
                    send_sem=ow_sent,
                    recv_sem=ow_come.at[shard],
                    device_id={"fsdp": mate(k, core) if k else partner},
                    device_id_type=MESH,
                ).start()

        (tile,) = q_tiles(step)
        gather(pairs + step, (tile,))

        @pl.when(step < pairs - 1)
        def _():
            hand_on(pairs + step + 1, q_tiles(step + 1))

        queries = project(tile) * score_scale
        upper, lower = queries[:half_tokens], queries[half_tokens:]
        first = 2 * q_pair(step)
        q_out[first] = jnp.where(low, upper, flip(lower)).astype(BF16)
        q_out[first + 1] = jnp.where(low, flip(upper), lower).astype(BF16)
        deliver(q_out, q_in, q_sent, q_come, first)
        deliver(q_out, q_in, q_sent, q_come, first + 1)
        return carry

    lax.fori_loop(0, pairs, q_step, 0)

    def ow_forward():
        for k in order:
            ow_wait(mate(k, core))
            pltpu.make_async_remote_copy(
                src_ref=ow_place(mate(k, core)),
                dst_ref=ow_place(mate(k, core)),
                send_sem=ow_sent,
                recv_sem=ow_come.at[mate(k, core)],
                device_id={"fsdp": partner},
                device_id_type=MESH,
            ).start()

    label_levels = levels - LANES // 2

    def token_rows(source):
        return pl.ds(pl.multiple_of(source * tokens, tokens), tokens)

    def label_hits(source):
        return jnp.where(label_levels == labels_in[source], 1.0, 0.0).T

    def widen(source, carry):
        @pl.when(source != me)
        def _():
            pltpu.make_async_copy(labels, labels_in.at[source], l_come.at[source]).wait()
            pltpu.make_async_copy(
                kv_out.at[source], kv_in.at[source], kv_come.at[source]
            ).wait()

        other = jnp.where(label_hits(source) > 0.5, 0.0, floor_score).astype(BF16)
        k_aug[token_rows(source), :] = jnp.where(low_full, kv_in[source], other)
        return carry

    lax.fori_loop(0, ring, widen, 0)

    everything = ring * tokens

    def attend(i, carry):
        source = lax.rem(me + near_then_far(ring, 7, i), ring)

        @pl.when(i == 1)
        def _():
            ow_forward()

        @pl.when(i > 0)
        def _():
            pltpu.make_async_copy(q_out.at[source], q_in.at[source], q_come.at[source]).wait()

        block = q_in[source].astype(F32)
        hits = label_hits(source)
        halves = (
            jnp.where(low, block, hits[:half_tokens]).astype(BF16),
            jnp.where(low, flip(block), hits[half_tokens:]).astype(BF16),
        )

        def score(half):
            part = lax.dot_general(
                halves[half],
                k_aug[...],
                (((1,), (1,)), ((), ())),
                preferred_element_type=F32,
            )
            scores[pl.ds(half * half_tokens, half_tokens), :] = part
            highest = part[:, :LANES]
            for t in range(1, everything // LANES):
                highest = jnp.maximum(highest, part[:, t * LANES : (t + 1) * LANES])
            return jnp.max(highest, axis=-1, keepdims=True)

        def mix(half, top):
            raised = jnp.exp(scores[pl.ds(half * half_tokens, half_tokens), :] - top)
            sums = raised[:, :LANES]
            for t in range(1, everything // LANES):
                sums = sums + raised[:, t * LANES : (t + 1) * LANES]
            mixed = jnp.dot(
                raised.astype(BF16),
                kv_in[...].reshape(everything, LANES),
                preferred_element_type=F32,
            )
            return mixed / jnp.sum(sums, axis=-1, keepdims=True)

        top = score(0)
        next_top = score(1)
        upper = mix(0, top)
        lower = mix(1, next_top)
        c_out[source] = jnp.where(low, flip(upper), lower).astype(BF16)
        deliver(c_out, c_in, c_sent, c_come, source)
        return carry

    lax.fori_loop(0, ring, attend, 0)

    ow_wait(partner)
    for k in order:
        ow_wait(mate(k, 1 - core))

    wide = 256

    def finish(step, carry):
        pair = q_pair(step)
        for head in (2 * pair, 2 * pair + 1):

            @pl.when(head != me)
            def _():
                pltpu.make_async_copy(c_out.at[head], c_in.at[head], c_come.at[head]).wait()

        left = c_in[2 * pair].astype(F32)
        right = c_in[2 * pair + 1].astype(F32)
        context = jnp.concatenate(
            [jnp.where(low, left, flip(right)), jnp.where(low, flip(left), right)], axis=0
        ).astype(BF16)
        for start in range(0, width, wide):
            place = pl.ds(start, wide)
            embedded[:, place] += jnp.dot(
                context, ow_all[columns(pair), place], preferred_element_type=F32
            )
        return carry

    lax.fori_loop(0, pairs, finish, 0)
    out[...] = embedded[...].astype(BF16)

    place = w_all.at[pl.ds(0, (2 * chips - 1) * depth), :]
    pltpu.make_async_copy(place, place, w_sent).wait()
    place = ow_all.at[:, pl.ds(0, (2 * chips - 1) * LANES)]
    pltpu.make_async_copy(place, place, ow_sent).wait()
    for buffer, sent in ((kv_out, kv_sent), (q_out, q_sent), (c_out, c_sent), (labels_in, l_sent)):
        place = buffer.at[pl.ds(0, ring - 1)]
        pltpu.make_async_copy(place, place, sent).wait()


def body(
    ring,
    shards,
    patches,
    segment_ids,
    patch_rows,
    patch_cols,
    row_table,
    col_table,
    norm_gain,
    qkv_weight,
    out_weight,
):
    _, tokens, width = patches.shape
    pairs = width // LANES
    dma = pltpu.SemaphoreType.DMA
    result = pl.pallas_call(
        functools.partial(block_kernel, ring, shards),
        out_shape=jax.ShapeDtypeStruct((tokens, width), BF16),
        in_specs=[pl.BlockSpec(memory_space=pltpu.HBM)] * 9,
        out_specs=pl.BlockSpec(memory_space=pltpu.VMEM),
        scratch_shapes=[
            pltpu.VMEM((tokens, width), BF16),
            pltpu.VMEM((1, tokens), jnp.int32),
            pltpu.VMEM((1, tokens), jnp.int32),
            pltpu.VMEM((1, tokens), jnp.int32),
            pltpu.VMEM((2 * row_table.shape[0], width), BF16),
            pltpu.VMEM((1, width), F32),
            dma((9,)),
            pltpu.VMEM((width, 3 * width), BF16),
            pltpu.VMEM((width, width), BF16),
            pltpu.VMEM((tokens, LANES), BF16),
            pltpu.VMEM((tokens, width), F32),
            pltpu.VMEM((tokens, width), BF16),
            pltpu.VMEM((ring, tokens, LANES), BF16),
            pltpu.VMEM((ring, tokens, LANES), BF16),
            pltpu.VMEM((ring, tokens // 2, LANES), BF16),
            pltpu.VMEM((ring, tokens // 2, LANES), BF16),
            pltpu.VMEM((ring, tokens // 2, LANES), BF16),
            pltpu.VMEM((ring, tokens // 2, LANES), BF16),
            pltpu.VMEM((ring, 1, tokens), jnp.int32),
            pltpu.VMEM((ring * tokens, LANES), BF16),
            pltpu.VMEM((tokens, ring * tokens), F32),
            dma,
            dma((2 * pairs,)),
            dma((2 * pairs,)),
            dma,
            dma((shards,)),
            dma,
            dma((ring,)),
            dma,
            dma((ring,)),
            dma,
            dma((ring,)),
            dma,
            dma((ring,)),
            pltpu.SemaphoreType.REGULAR,
            pltpu.SemaphoreType.REGULAR((pairs,)),
        ],
        compiler_params=pltpu.CompilerParams(
            collective_id=0, has_side_effects=True, vmem_limit_bytes=60 << 20
        ),
        name="encoder_block",
    )(
        patches[0],
        segment_ids,
        patch_rows,
        patch_cols,
        row_table,
        col_table,
        norm_gain[None],
        qkv_weight,
        out_weight,
    )
    return result[None]


def solution(mesh):
    ring, shards = mesh.shape["ctx"], mesh.shape["fsdp"]
    tokens_spec = P(("groups", "fsdp"), "ctx")
    placed = (
        P(("groups", "fsdp"), "ctx", None),
        tokens_spec,
        tokens_spec,
        tokens_spec,
        P(),
        P(),
        P(),
        P("fsdp", None),
        P(None, "fsdp"),
    )
    return jax.shard_map(
        functools.partial(body, ring, shards),
        mesh=mesh,
        in_specs=placed,
        out_specs=P(("groups", "fsdp"), "ctx", None),
        check_vma=False,
    )
```

```python
import functools

import jax
import jax.numpy as jnp
from jax import lax
from jax.experimental import pallas as pl
from jax.experimental.pallas import tpu as pltpu
from jax.sharding import PartitionSpec as P

HEADS = 16
LANES = 128
epsilon = 1e-06
floor_score = -1e30
MESH = pl.DeviceIdType.MESH
F32 = jnp.float32
BF16 = jnp.bfloat16


def flip(value):
    return pltpu.roll(value, LANES // 2, 1)


def far_first(count, step):
    odd = lax.rem(step, 2)
    return count // 2 + (1 - odd) * (step // 2) - odd * ((step + 1) // 2)


def block_kernel(
    ring,
    shards,
    patches_in,
    labels_at,
    rows_at,
    cols_at,
    row_table_in,
    col_table_in,
    gain_in,
    w_in,
    ow_in,
    out,
    patches,
    labels,
    patch_rows,
    patch_cols,
    table,
    gain,
    loaded,
    w_all,
    ow_all,
    onehots,
    normed,
    kv_out,
    kv_in,
    q_out,
    q_in,
    c_out,
    c_in,
    labels_in,
    k_aug,
    scores,
    w_sent,
    mates_come,
    partner_come,
    ow_sent,
    ow_come,
    kv_sent,
    kv_come,
    q_sent,
    q_come,
    c_sent,
    c_come,
    l_sent,
    l_come,
    row_here,
    pair_here,
):
    tokens, width = patches.shape
    half_tokens = tokens // 2
    depth = w_in.shape[0]
    pairs = width // LANES
    chips = shards // 2
    me = lax.axis_index("ctx")
    shard = lax.axis_index("fsdp")
    chip, core = shard // 2, lax.rem(shard, 2)
    own_pair = me // 2
    partner = 2 * chip + 1 - core

    def mate(k, which):
        return 2 * lax.rem(chip + k, chips) + which

    def columns(tile):
        return pl.ds(pl.multiple_of(tile * LANES, LANES), LANES)

    def w_rows(source):
        return pl.ds(pl.multiple_of(source * depth, depth), depth)

    def ow_place(source):
        return ow_all.at[:, columns(source)]

    grid_size = row_table_in.shape[0]
    loads = [
        pltpu.make_async_copy(source, target, loaded.at[k])
        for k, (source, target) in enumerate(
            (
                (w_in, w_all.at[w_rows(shard), :]),
                (rows_at, patch_rows),
                (cols_at, patch_cols),
                (row_table_in, table.at[pl.ds(0, grid_size), :]),
                (col_table_in, table.at[pl.ds(grid_size, grid_size), :]),
                (patches_in, patches),
                (gain_in, gain),
                (labels_at, labels),
                (ow_in, ow_place(shard)),
            )
        )
    ]
    for load in loads:
        load.start()

    barrier = pltpu.get_barrier_semaphore()

    def signal(semaphore, **where):
        pl.semaphore_signal(semaphore, inc=1, device_id=where, device_id_type=MESH)

    @pl.when(shard == 0)
    def _():
        pl.semaphore_wait(barrier, shards - 1)
        for other in range(1, shards):
            signal(row_here, fsdp=other)

    @pl.when(shard > 0)
    def _():
        signal(barrier, fsdp=0)
        pl.semaphore_wait(row_here, 1)

    @pl.when(shard > 0)
    def _():
        start = 2 * lax.rem(own_pair + pairs - shard, pairs)
        signal(barrier, ctx=start)
        signal(barrier, ctx=start + 1)

    @pl.when(shard == shards - 1)
    def _():
        signal(barrier, ctx=4 * own_pair + 1 - me)

    def kv_ahead(step):
        return far_first(pairs, jnp.where(step < 2, 1 - step, step))

    def meet(step):
        ahead = kv_ahead(step)

        @pl.when((shard == ahead) & (shard > 0))
        def _():
            pl.semaphore_wait(barrier, jnp.where(shard == shards - 1, 3, 2))
            for k in range(1, shards):
                signal(pair_here.at[ahead], fsdp=lax.rem(shard + k, shards))

    def met(step):
        ahead = kv_ahead(step)

        @pl.when((shard != ahead) & (ahead > 0))
        def _():
            pl.semaphore_wait(pair_here.at[ahead], 1)

    lane = lax.broadcasted_iota(jnp.int32, (half_tokens, LANES), 1)
    low = lane < LANES // 2
    lane_full = lax.broadcasted_iota(jnp.int32, (tokens, LANES), 1)
    low_full = lane_full < LANES // 2

    def pair_of(step):
        return lax.rem(own_pair + kv_ahead(step), pairs)

    def kv_tiles(step):
        return pairs + pair_of(step), 2 * pairs + pair_of(step)

    def near_then_far(count, near, step):
        return jnp.where(
            step < near, far_first(count, count - 1 - step), far_first(count, step - near)
        )

    def q_pair(step):
        return lax.rem(own_pair + near_then_far(pairs, 3, step), pairs)

    def q_tiles(step):
        return (q_pair(step),)

    order = [2, 1, 3] if chips == 4 else list(range(1, chips))

    def w_copy(source, tile, come, target):
        place = w_all.at[w_rows(source), columns(tile)]
        pltpu.make_async_remote_copy(
            src_ref=place,
            dst_ref=place,
            send_sem=w_sent,
            recv_sem=come,
            device_id={"fsdp": target},
            device_id_type=MESH,
        ).start()

    def spread(number, tiles):
        for k in order:
            for tile in tiles:
                w_copy(shard, tile, mates_come.at[number], mate(k, core))
        for tile in tiles:
            w_copy(shard, tile, partner_come.at[number], partner)

    def w_wait(come, blocks, tiles):
        place = w_all.at[pl.ds(0, blocks * depth), pl.ds(0, len(tiles) * LANES)]
        pltpu.make_async_copy(place, place, come).wait()

    def hand_on(number, tiles):
        w_wait(mates_come.at[number], chips - 1, tiles)
        for k in order:
            for tile in tiles:
                w_copy(mate(k, core), tile, partner_come.at[number], partner)

    def gather(number, tiles):
        w_wait(partner_come.at[number], chips, tiles)

    loads[0].wait()
    for step in range(3):
        spread(step, kv_tiles(step))

    def tell_labels(target):
        @pl.when(target != me)
        def _():
            pltpu.make_async_remote_copy(
                src_ref=labels,
                dst_ref=labels_in.at[me],
                send_sem=l_sent,
                recv_sem=l_come.at[me],
                device_id={"ctx": target},
                device_id_type=MESH,
            ).start()

    levels = lax.broadcasted_iota(jnp.int32, (LANES, tokens), 0)
    for load in loads[1:]:
        load.wait()
    labels_in[me] = labels[...]
    hit = (levels == patch_rows[...]) | (levels == patch_cols[...] + grid_size)
    onehots[...] = jnp.where(hit, 1.0, 0.0).T.astype(BF16)
    scale = gain[...]
    strip = 64

    def embed(i, carry):
        rows = pl.ds(pl.multiple_of(i * strip, strip), strip)
        value = patches[rows, :].astype(F32) + jnp.dot(
            onehots[rows, :], table[...], preferred_element_type=F32
        )
        out[rows, :] = value
        average = jnp.mean(value, axis=-1, keepdims=True)
        centered = value - average
        variance = jnp.mean(centered * centered, axis=-1, keepdims=True)
        normed[rows, :] = (centered * lax.rsqrt(variance + epsilon) * scale).astype(BF16)
        return carry

    lax.fori_loop(0, tokens // strip, embed, 0)

    def project(tile):
        return jnp.dot(normed[...], w_all[:, columns(tile)], preferred_element_type=F32)

    def deliver(outgoing, incoming, sent, come, target):
        @pl.when(target != me)
        def _():
            pltpu.make_async_remote_copy(
                src_ref=outgoing.at[target],
                dst_ref=incoming.at[me],
                send_sem=sent,
                recv_sem=come.at[me],
                device_id={"ctx": target},
                device_id_type=MESH,
            ).start()

        @pl.when(target == me)
        def _():
            incoming[me] = outgoing[target]

    hand_on(0, kv_tiles(0))
    meet(0)

    def kv_step(step, carry):
        @pl.when(step < pairs - 3)
        def _():
            spread(step + 3, kv_tiles(step + 3))

        @pl.when(step >= pairs - 3)
        def _():
            spread(step + 3, q_tiles(step + 3 - pairs))

        def next_on():
            @pl.when(step < pairs - 1)
            def _():
                hand_on(step + 1, kv_tiles(step + 1))

            @pl.when(step == pairs - 1)
            def _():
                hand_on(pairs, q_tiles(0))

        k_tile, v_tile = kv_tiles(step)
        gather(step, (k_tile, v_tile))

        @pl.when(step > 0)
        def _():
            next_on()

        keys = project(k_tile)
        values = project(v_tile)
        first = 2 * pair_of(step)
        kv_out[first] = jnp.where(low_full, keys, flip(values)).astype(BF16)
        kv_out[first + 1] = jnp.where(low_full, flip(keys), values).astype(BF16)
        met(step)
        for target in (first, first + 1):
            tell_labels(target)
            deliver(kv_out, kv_in, kv_sent, kv_come, target)

        @pl.when(step == 0)
        def _():
            next_on()

        @pl.when(step < pairs - 1)
        def _():
            meet(step + 1)

        return carry

    lax.fori_loop(0, pairs, kv_step, 0)

    def ow_wait(source):
        pltpu.make_async_copy(ow_place(source), ow_place(source), ow_come.at[source]).wait()

    score_scale = 1.0 / (LANES // 2) ** 0.5

    def q_step(step, carry):
        @pl.when(step < pairs - 3)
        def _():
            spread(pairs + step + 3, q_tiles(step + 3))

        @pl.when(step == pairs - 3)
        def _():
            for k in order + [0]:
                pltpu.make_async_remote_copy(
                    src_ref=ow_place(shard),
                    dst_ref=ow_place(shard),
                    send_sem=ow_sent,
                    recv_sem=ow_come.at[shard],
                    device_id={"fsdp": mate(k, core) if k else partner},
                    device_id_type=MESH,
                ).start()

        (tile,) = q_tiles(step)
        gather(pairs + step, (tile,))

        @pl.when(step < pairs - 1)
        def _():
            hand_on(pairs + step + 1, q_tiles(step + 1))

        queries = project(tile) * score_scale
        upper, lower = queries[:half_tokens], queries[half_tokens:]
        first = 2 * q_pair(step)
        q_out[first] = jnp.where(low, upper, flip(lower)).astype(BF16)
        q_out[first + 1] = jnp.where(low, flip(upper), lower).astype(BF16)
        deliver(q_out, q_in, q_sent, q_come, first)
        deliver(q_out, q_in, q_sent, q_come, first + 1)
        return carry

    lax.fori_loop(0, pairs, q_step, 0)

    def ow_forward():
        for k in order:
            ow_wait(mate(k, core))
            pltpu.make_async_remote_copy(
                src_ref=ow_place(mate(k, core)),
                dst_ref=ow_place(mate(k, core)),
                send_sem=ow_sent,
                recv_sem=ow_come.at[mate(k, core)],
                device_id={"fsdp": partner},
                device_id_type=MESH,
            ).start()

    label_levels = levels - LANES // 2

    def token_rows(source):
        return pl.ds(pl.multiple_of(source * tokens, tokens), tokens)

    def label_hits(source):
        return jnp.where(label_levels == labels_in[source], 1.0, 0.0).T

    def widen(source, carry):
        @pl.when(source != me)
        def _():
            pltpu.make_async_copy(labels, labels_in.at[source], l_come.at[source]).wait()
            pltpu.make_async_copy(
                kv_out.at[source], kv_in.at[source], kv_come.at[source]
            ).wait()

        other = jnp.where(label_hits(source) > 0.5, 0.0, floor_score).astype(BF16)
        k_aug[token_rows(source), :] = jnp.where(low_full, kv_in[source], other)
        return carry

    lax.fori_loop(0, ring, widen, 0)

    everything = ring * tokens

    def attend(i, carry):
        source = lax.rem(me + near_then_far(ring, 7, i), ring)

        @pl.when(i == 1)
        def _():
            ow_forward()

        @pl.when(i > 0)
        def _():
            pltpu.make_async_copy(q_out.at[source], q_in.at[source], q_come.at[source]).wait()

        block = q_in[source].astype(F32)
        hits = label_hits(source)
        halves = (
            jnp.where(low, block, hits[:half_tokens]).astype(BF16),
            jnp.where(low, flip(block), hits[half_tokens:]).astype(BF16),
        )

        def score(half):
            part = lax.dot_general(
                halves[half],
                k_aug[...],
                (((1,), (1,)), ((), ())),
                preferred_element_type=F32,
            )
            scores[pl.ds(half * half_tokens, half_tokens), :] = part
            highest = part[:, :LANES]
            for t in range(1, everything // LANES):
                highest = jnp.maximum(highest, part[:, t * LANES : (t + 1) * LANES])
            return jnp.max(highest, axis=-1, keepdims=True)

        def mix(half, top):
            raised = jnp.exp(scores[pl.ds(half * half_tokens, half_tokens), :] - top)
            sums = raised[:, :LANES]
            for t in range(1, everything // LANES):
                sums = sums + raised[:, t * LANES : (t + 1) * LANES]
            mixed = jnp.dot(
                raised.astype(BF16),
                kv_in[...].reshape(everything, LANES),
                preferred_element_type=F32,
            )
            return mixed / jnp.sum(sums, axis=-1, keepdims=True)

        top = score(0)
        next_top = score(1)
        upper = mix(0, top)
        lower = mix(1, next_top)
        c_out[source] = jnp.where(low, flip(upper), lower).astype(BF16)
        deliver(c_out, c_in, c_sent, c_come, source)
        return carry

    lax.fori_loop(0, ring, attend, 0)

    ow_wait(partner)
    for k in order:
        ow_wait(mate(k, 1 - core))

    wide = 256

    def finish(step, carry):
        pair = q_pair(step)
        for head in (2 * pair, 2 * pair + 1):

            @pl.when(head != me)
            def _():
                pltpu.make_async_copy(c_out.at[head], c_in.at[head], c_come.at[head]).wait()

        left = c_in[2 * pair].astype(F32)
        right = c_in[2 * pair + 1].astype(F32)
        context = jnp.concatenate(
            [jnp.where(low, left, flip(right)), jnp.where(low, flip(left), right)], axis=0
        ).astype(BF16)
        for start in range(0, width, wide):
            place = pl.ds(start, wide)
            out[:, place] += jnp.dot(
                context, ow_all[columns(pair), place], preferred_element_type=F32
            )
        return carry

    lax.fori_loop(0, pairs, finish, 0)

    place = w_all.at[pl.ds(0, (2 * chips - 1) * depth), :]
    pltpu.make_async_copy(place, place, w_sent).wait()
    place = ow_all.at[:, pl.ds(0, (2 * chips - 1) * LANES)]
    pltpu.make_async_copy(place, place, ow_sent).wait()
    for buffer, sent in ((kv_out, kv_sent), (q_out, q_sent), (c_out, c_sent), (labels_in, l_sent)):
        place = buffer.at[pl.ds(0, ring - 1)]
        pltpu.make_async_copy(place, place, sent).wait()


def body(
    ring,
    shards,
    patches,
    segment_ids,
    patch_rows,
    patch_cols,
    row_table,
    col_table,
    norm_gain,
    qkv_weight,
    out_weight,
):
    _, tokens, width = patches.shape
    pairs = width // LANES
    dma = pltpu.SemaphoreType.DMA
    result = pl.pallas_call(
        functools.partial(block_kernel, ring, shards),
        out_shape=jax.ShapeDtypeStruct((tokens, width), F32),
        in_specs=[pl.BlockSpec(memory_space=pltpu.HBM)] * 9,
        out_specs=pl.BlockSpec(memory_space=pltpu.VMEM),
        scratch_shapes=[
            pltpu.VMEM((tokens, width), BF16),
            pltpu.VMEM((1, tokens), jnp.int32),
            pltpu.VMEM((1, tokens), jnp.int32),
            pltpu.VMEM((1, tokens), jnp.int32),
            pltpu.VMEM((2 * row_table.shape[0], width), BF16),
            pltpu.VMEM((1, width), F32),
            dma((9,)),
            pltpu.VMEM((width, 3 * width), BF16),
            pltpu.VMEM((width, width), BF16),
            pltpu.VMEM((tokens, LANES), BF16),
            pltpu.VMEM((tokens, width), BF16),
            pltpu.VMEM((ring, tokens, LANES), BF16),
            pltpu.VMEM((ring, tokens, LANES), BF16),
            pltpu.VMEM((ring, tokens // 2, LANES), BF16),
            pltpu.VMEM((ring, tokens // 2, LANES), BF16),
            pltpu.VMEM((ring, tokens // 2, LANES), BF16),
            pltpu.VMEM((ring, tokens // 2, LANES), BF16),
            pltpu.VMEM((ring, 1, tokens), jnp.int32),
            pltpu.VMEM((ring * tokens, LANES), BF16),
            pltpu.VMEM((tokens, ring * tokens), F32),
            dma,
            dma((2 * pairs,)),
            dma((2 * pairs,)),
            dma,
            dma((shards,)),
            dma,
            dma((ring,)),
            dma,
            dma((ring,)),
            dma,
            dma((ring,)),
            dma,
            dma((ring,)),
            pltpu.SemaphoreType.REGULAR,
            pltpu.SemaphoreType.REGULAR((pairs,)),
        ],
        compiler_params=pltpu.CompilerParams(
            collective_id=0, has_side_effects=True, vmem_limit_bytes=60 << 20
        ),
        name="encoder_block",
    )(
        patches[0],
        segment_ids,
        patch_rows,
        patch_cols,
        row_table,
        col_table,
        norm_gain[None],
        qkv_weight,
        out_weight,
    )
    return result.astype(BF16)[None]


def solution(mesh):
    ring, shards = mesh.shape["ctx"], mesh.shape["fsdp"]
    tokens_spec = P(("groups", "fsdp"), "ctx")
    placed = (
        P(("groups", "fsdp"), "ctx", None),
        tokens_spec,
        tokens_spec,
        tokens_spec,
        P(),
        P(),
        P(),
        P("fsdp", None),
        P(None, "fsdp"),
    )
    return jax.shard_map(
        functools.partial(body, ring, shards),
        mesh=mesh,
        in_specs=placed,
        out_specs=P(("groups", "fsdp"), "ctx", None),
        check_vma=False,
    )
```
